32 devices in a mesh: seq: 8 (over y, x, core), chan: 4 (over z).
Axes of the slice: x: 2, y: 2, z: 4, core: 2. Of those that a mesh axis runs over, the one named last changes fastest.
Arguments:
- fwd_q: bfloat16 [1024, 4096], P('seq', 'chan'), may hold values from -6 to 6
- fwd_k: bfloat16 [1024, 4096], P('seq', 'chan'), may hold values from -6 to 6
- fwd_v: bfloat16 [1024, 4096], P('seq', 'chan'), may hold values from -6 to 6
- bwd_q: bfloat16 [1024, 4096], P('seq', 'chan'), may hold values from -6 to 6
- bwd_k: bfloat16 [1024, 4096], P('seq', 'chan'), may hold values from -6 to 6
- bwd_v: bfloat16 [1024, 4096], P('seq', 'chan'), may hold values from -6 to 6
- bwd_grad: bfloat16 [1024, 4096], P('seq', 'chan'), may hold values from -6 to 6
- filters: float32 [1024, 1024], P('seq', 'chan'), may hold values from -0.1875 to 0.1875
- skip: float32 [4096], P('chan'), may hold values from -4 to 4
Outputs:
- output: bfloat16 [1024, 4096], P('seq', 'chan')
- grad_query: bfloat16 [1024, 4096], P('seq', 'chan')
- grad_key: bfloat16 [1024, 4096], P('seq', 'chan')
- grad_value: bfloat16 [1024, 4096], P('seq', 'chan')
- grad_filter: float32 [1024, 1024], P('seq', 'chan')
- grad_skip: float32 [4096], P('chan')
The draws below stay inside these ranges and needn't reach their ends.
All inputs are finite; a program needn't handle non-finite values.
Results may differ from the reference program's by a relative error of at most 0.0075.
Values may be sent and summed in bfloat16 or wider, within the bound.
A program may use at most 256 MiB of HBM per device.

```python
import math
import jax
import jax.numpy as jnp
from jax import lax

C = 4096
FILTERS = 1024
SEQ_LEN = 1024


def block_scale(key, shape, shards, smallest, top_value):
    gain, own = 1.0, jax.random.fold_in(key, 6)
    for position, shards_of in shards:
        draws = jnp.exp(jax.random.uniform(jax.random.fold_in(own, position), (shards_of,), jnp.float32, smallest / len(shards), top_value / len(shards)))
        gain = gain * jnp.repeat(draws, shape[position] // shards_of).reshape([-1 if axis == position else 1 for axis in range(len(shape))])
    return gain


def bell_draw(own_key, extent, scale, limit, shards=(), kind=jnp.bfloat16):
    drawn = jax.random.normal(own_key, extent, jnp.float32) * scale
    if len(shards) > 0:
        drawn = block_scale(own_key, extent, shards, -0.22, 0.18) * drawn
    return jnp.clip(drawn, min=-limit, max=limit).astype(kind)


def setup_inputs(seed: int = 0) -> dict:
    streams_of = jax.random.split(jax.random.key(seed), 10)
    fwd_q = bell_draw(streams_of[0], (SEQ_LEN, C), 1.0, 6.0, ((0, 8), (1, 4)))
    fwd_k = bell_draw(streams_of[1], (SEQ_LEN, C), 1.0, 6.0, ((0, 8), (1, 4)))
    fwd_v = bell_draw(streams_of[2], (SEQ_LEN, C), 1.0, 6.0, ((0, 8), (1, 4)))
    bwd_q = bell_draw(streams_of[3], (SEQ_LEN, C), 1.0, 6.0, ((0, 8), (1, 4)))
    bwd_k = bell_draw(streams_of[4], (SEQ_LEN, C), 1.0, 6.0, ((0, 8), (1, 4)))
    bwd_v = bell_draw(streams_of[5], (SEQ_LEN, C), 1.0, 6.0, ((0, 8), (1, 4)))
    bwd_grad = bell_draw(streams_of[6], (SEQ_LEN, C), 1.0, 6.0, ((0, 8), (1, 4)))
    filters = bell_draw(streams_of[7], (SEQ_LEN, FILTERS), SEQ_LEN ** -0.5, 0.1875, ((0, 8), (1, 4)), jnp.float32)
    skip = bell_draw(streams_of[8], (C,), 1.0, 4.0, ((0, 4),), jnp.float32)
    return {"fwd_q": fwd_q, "fwd_k": fwd_k, "fwd_v": fwd_v, "bwd_q": bwd_q, "bwd_k": bwd_k, "bwd_v": bwd_v, "bwd_grad": bwd_grad, "filters": filters, "skip": skip}


def spectrum(values):
    return jnp.fft.rfft(values, n=2 * values.shape[0], axis=0)

def signal(spec, seq_length):
    return jnp.fft.irfft(spec, n=2 * seq_length, axis=0)[:seq_length]

def rounded(values):
    return lax.optimization_barrier(values.astype(jnp.bfloat16)).astype(jnp.float32)

def reference(fwd_q, fwd_k, fwd_v, bwd_q, bwd_k, bwd_v, bwd_grad, filters, skip):
    seq_length, channels = fwd_q.shape
    filter_count = filters.shape[1]
    grad_scale = 1.0 / math.sqrt(seq_length)
    filter_spec = spectrum(filters.astype(jnp.float32))
    out_parts, query_parts, key_parts, value_parts, skip_parts = ([], [], [], [], [])
    filter_total = jnp.zeros((seq_length, filter_count), jnp.float32)
    for group_index in range(channels // filter_count):
        start_col = group_index * filter_count
        stop_col = start_col + filter_count

        def column_block(array):
            return array[:, start_col:stop_col].astype(jnp.float32)
        skip_gain = skip[start_col:stop_col].astype(jnp.float32)
        source = rounded(column_block(fwd_k) * column_block(fwd_v))
        mixed = signal(filter_spec * spectrum(source), seq_length) + skip_gain * source
        out_parts.append((column_block(fwd_q) * mixed).astype(jnp.bfloat16))
        second_source = rounded(column_block(bwd_k) * column_block(bwd_v))
        second_spec = spectrum(second_source)
        mixed_two = signal(filter_spec * second_spec, seq_length) + skip_gain * second_source
        query_parts.append((column_block(bwd_grad) * mixed_two).astype(jnp.bfloat16))
        upstream = rounded(column_block(bwd_grad) * column_block(bwd_q))
        upstream_spec = spectrum(upstream)
        through = signal(jnp.conj(filter_spec) * upstream_spec, seq_length) + skip_gain * upstream
        key_parts.append((through * column_block(bwd_v)).astype(jnp.bfloat16))
        value_parts.append((through * column_block(bwd_k)).astype(jnp.bfloat16))
        filter_total = filter_total + signal(jnp.conj(second_spec) * upstream_spec, seq_length) * grad_scale
        skip_parts.append(lax.optimization_barrier(jnp.sum(upstream * second_source, axis=0)) * grad_scale)
    return (jnp.concatenate(out_parts, axis=1), jnp.concatenate(query_parts, axis=1), jnp.concatenate(key_parts, axis=1), jnp.concatenate(value_parts, axis=1), filter_total, jnp.concatenate(skip_parts, axis=0))
```

```python
import functools
import math

import jax
import jax.numpy as jnp
import numpy as np
from jax import lax
from jax.experimental import pallas as pl
from jax.experimental.pallas import tpu as pltpu
from jax.sharding import PartitionSpec as P

HIGHEST = lax.Precision.HIGHEST
LANES = 128
MESH = pl.DeviceIdType.MESH
BF16 = jnp.bfloat16
F32 = jnp.float32


def index_ramp(total):
    return jnp.arange(total, dtype=jnp.int32)


def widened(values):
    return values.astype(jnp.float32)


def angles(out_index, in_index, period, sign):
    phase_steps = out_index[:, None] * in_index[None, :] % period
    phase = phase_steps.astype(jnp.float32) * (sign * 2.0 * math.pi / period)
    return (jnp.cos(phase), jnp.sin(phase))


def times_table(left, right):
    return (left[0] * right[0] - left[1] * right[1], left[0] * right[1] + left[1] * right[0])


def block_table(pair):
    cosine, sine_part = pair
    return jnp.stack([jnp.stack([cosine, -sine_part]), jnp.stack([sine_part, cosine])])


def product_of(left, right):
    return jnp.stack(
        [left[0] * right[0] - left[1] * right[1], left[0] * right[1] + left[1] * right[0]]
    )


def conj_product(left, right):
    return jnp.stack(
        [left[0] * right[0] + left[1] * right[1], left[0] * right[1] - left[1] * right[0]]
    )


def joined(left, right):
    return jnp.concatenate([left, right], axis=-1)


def factor(total):
    chosen = 1
    for candidate in range(1, total + 1):
        if candidate * candidate <= total and total % candidate == 0:
            chosen = candidate
    return chosen


def leading_section(values, seq_size):
    cosine, sine_part = angles(index_ramp(2 * seq_size), index_ramp(seq_size), 2 * seq_size, -1.0)
    table = jnp.stack([cosine, sine_part])
    return jnp.einsum("rkp,pmc->rkmc", table, values, precision=HIGHEST)


def trailing_section(values, seq_size, period):
    cosine, sine_part = angles(index_ramp(seq_size), index_ramp(2 * seq_size), 2 * seq_size, 1.0)
    table = jnp.stack([cosine, -sine_part]) * (1.0 / period)
    return jnp.einsum("rpk,rkmc->pmc", table, values, precision=HIGHEST)


def inner_forward(values, freq_keys, period):
    lead_size, row_count, chan_count = values.shape[1:]
    outer_size = factor(row_count)
    inner_size = row_count // outer_size
    values = values.reshape(2, lead_size, outer_size, inner_size, chan_count)
    first_twiddle = angles(freq_keys, index_ramp(row_count), period, -1.0)
    first_twiddle = tuple(
        (part.reshape(lead_size, outer_size, inner_size) for part in first_twiddle)
    )
    outer_dft = angles(index_ramp(outer_size), index_ramp(outer_size), outer_size, -1.0)
    outer_table = times_table(
        tuple((part[None, :, :, None] for part in outer_dft)),
        tuple((part[:, None, :, :] for part in first_twiddle)),
    )
    values = jnp.einsum("rsjxab,sjabc->rjxbc", block_table(outer_table), values, precision=HIGHEST)
    second_twiddle = angles(index_ramp(outer_size), index_ramp(inner_size), row_count, -1.0)
    inner_dft = angles(index_ramp(inner_size), index_ramp(inner_size), inner_size, -1.0)
    inner_table = times_table(
        tuple((part[None, :, :] for part in inner_dft)),
        tuple((part[:, None, :] for part in second_twiddle)),
    )
    return jnp.einsum("rsxyb,sjxbc->rjxyc", block_table(inner_table), values, precision=HIGHEST)


def inner_inverse(values, freq_keys, period):
    lead_size, outer_size, inner_size, chan_count = values.shape[1:]
    row_count = outer_size * inner_size
    second_twiddle = angles(index_ramp(outer_size), index_ramp(inner_size), row_count, 1.0)
    inner_dft = angles(index_ramp(inner_size), index_ramp(inner_size), inner_size, 1.0)
    inner_table = times_table(
        tuple((part[:, :, None] for part in second_twiddle)),
        tuple((part[None, :, :] for part in inner_dft)),
    )
    values = jnp.einsum("rsxby,sjxyc->rjxbc", block_table(inner_table), values, precision=HIGHEST)
    first_twiddle = angles(freq_keys, index_ramp(row_count), period, 1.0)
    first_twiddle = tuple(
        (part.reshape(lead_size, outer_size, inner_size) for part in first_twiddle)
    )
    outer_dft = angles(index_ramp(outer_size), index_ramp(outer_size), outer_size, 1.0)
    outer_table = times_table(
        tuple((part[:, :, :, None] for part in first_twiddle)),
        tuple((part[None, :, None, :] for part in outer_dft)),
    )
    values = jnp.einsum("rsjabx,sjxbc->rjabc", block_table(outer_table), values, precision=HIGHEST)
    return values.reshape(2, lead_size, row_count, chan_count)


def forward_local(signal_part, seq_size):
    seq_length, chan_count = signal_part.shape
    row_count = seq_length // seq_size
    values = leading_section(signal_part.reshape(seq_size, row_count, chan_count), seq_size)
    return inner_forward(values, index_ramp(2 * seq_size), 2 * seq_length)


def inverse_local(values, seq_size):
    lead_size, outer_size, inner_size, chan_count = values.shape[1:]
    row_count = outer_size * inner_size
    period = 2 * seq_size * row_count
    values = inner_inverse(values, index_ramp(2 * seq_size), period)
    return trailing_section(values, seq_size, period).reshape(seq_size * row_count, chan_count)


def filter_times_pair(spec_filter, spec_pair):
    shape_pair = spec_pair.shape
    width = spec_filter.shape[-1]
    pair_view = spec_pair.reshape(shape_pair[:-1] + (2, width))
    filter_view = spec_filter[..., None, :]
    return product_of(filter_view, pair_view).reshape(shape_pair)


def per_device(fwd_q, fwd_k, fwd_v, bwd_q, bwd_k, bwd_v, bwd_grad, filters, skip):
    row_count, chan_width = fwd_q.shape
    seq_size = lax.axis_size("seq")
    grad_scale = 1.0 / math.sqrt(row_count * seq_size)
    source = (widened(fwd_k) * widened(fwd_v)).astype(jnp.bfloat16)
    second_source = (widened(bwd_k) * widened(bwd_v)).astype(jnp.bfloat16)
    upstream = (widened(bwd_grad) * widened(bwd_q)).astype(jnp.bfloat16)
    skip_gain = widened(skip)
    filters_all = lax.all_gather(filters, "chan", axis=1, tiled=True)
    narrow = chan_width // seq_size
    local_first, local_second = (
        lax.all_to_all(source, "seq", split_axis=1, concat_axis=0, tiled=True),
        lax.all_to_all(second_source, "seq", split_axis=1, concat_axis=0, tiled=True),
    )
    local_filter = lax.all_to_all(filters_all, "seq", split_axis=1, concat_axis=0, tiled=True)
    local_up = lax.all_to_all(upstream, "seq", split_axis=1, concat_axis=0, tiled=True)
    spec_sources = forward_local(
        widened(jnp.concatenate([local_first, local_second], axis=1)), seq_size
    )
    spec_filter = forward_local(local_filter, seq_size)
    conv_local = inverse_local(filter_times_pair(spec_filter, spec_sources), seq_size)
    conv_first, conv_second = (
        lax.all_to_all(conv_local[:, :narrow], "seq", split_axis=0, concat_axis=1, tiled=True),
        lax.all_to_all(conv_local[:, narrow:], "seq", split_axis=0, concat_axis=1, tiled=True),
    )
    spec_up = forward_local(widened(local_up), seq_size)
    spec_second = spec_sources[..., narrow:]
    back_local = inverse_local(
        joined(conj_product(spec_filter, spec_up), conj_product(spec_second, spec_up)), seq_size
    )
    through_conv, filter_terms = (
        lax.all_to_all(back_local[:, :narrow], "seq", split_axis=0, concat_axis=1, tiled=True),
        lax.all_to_all(
            back_local[:, narrow:] * grad_scale, "seq", split_axis=0, concat_axis=1, tiled=True
        ),
    )
    grad_filter = lax.psum_scatter(filter_terms, "chan", scatter_dimension=1, tiled=True)
    source_wide = widened(source)
    second_wide = widened(second_source)
    upstream_wide = widened(upstream)
    mixed = conv_first + skip_gain * source_wide
    output = (widened(fwd_q) * mixed).astype(jnp.bfloat16)
    mixed_two = conv_second + skip_gain * second_wide
    grad_query = (widened(bwd_grad) * mixed_two).astype(jnp.bfloat16)
    through = through_conv + skip_gain * upstream_wide
    grad_key = (through * widened(bwd_v)).astype(jnp.bfloat16)
    grad_value = (through * widened(bwd_k)).astype(jnp.bfloat16)
    grad_skip = lax.psum(jnp.sum(upstream_wide * second_wide, axis=0) * grad_scale, "seq")
    return (output, grad_query, grad_key, grad_value, grad_filter, grad_skip)


def block_tables(rows):
    freq = 2 * np.arange(rows)[:, None] + 1
    phase = (freq * np.arange(rows)[None, :] % (4 * rows)) * (np.pi / (2 * rows))
    forward = np.concatenate([np.cos(phase), -np.sin(phase)], axis=0)
    inverse = np.concatenate([np.cos(phase), -np.sin(phase)], axis=0).T / rows
    return forward.astype(np.float32), inverse.astype(np.float32)


def kernel(
    n, nc, scale,
    fq, fk, fv, bq, bk, bv, bg, filt, skip, fwd_t, inv_t,
    out_o, gq_o, gk_o, gv_o, gf_o, gs_o,
    su_send, s1_send, fz, su, s1, rf, spec_s, spec_u, spec_f, spec_w, prod,
    c_send, c_recv, g_send, rg, zg, k_send, k_recv,
    su_ss, su_rs, s1_ss, s1_rs, f_ss, f_rs, z_ss, z_rs, c_ss, c_rs, g_ss, g_rs, y_ss, y_rs, k_ss, k_rs,
):
    rows, chan_width = fq.shape
    w = chan_width // n
    per = filt.shape[1] // w
    me = lax.axis_index("seq")
    mz = lax.axis_index("chan")
    peers = [lax.rem(me + r, n) for r in range(1, n)]
    zpeers = [lax.rem(mz + r, nc) for r in range(1, nc)]
    started = []

    def lane(p):
        return pl.ds(pl.multiple_of(p * w, w), w)

    def copy(src, dst, ss, rs, to):
        return pltpu.make_async_remote_copy(
            src_ref=src, dst_ref=dst, send_sem=ss, recv_sem=rs, device_id=to, device_id_type=MESH
        )

    def send(src, dst, ss, rs, to):
        c = copy(src, dst, ss, rs, to)
        c.start()
        started.append(c)

    def arrived(buf, ss, rs, to):
        copy(buf, buf, ss, rs, to).wait_recv()

    barrier = pltpu.get_barrier_semaphore()
    for p in peers:
        pl.semaphore_signal(barrier, inc=1, device_id={"seq": p}, device_id_type=MESH)
    for z in zpeers:
        pl.semaphore_signal(barrier, inc=1, device_id={"chan": z}, device_id_type=MESH)

    for h in range(per):
        fz[mz * per + h] = filt[:, h * w:(h + 1) * w].astype(BF16)
    for p in range(n):
        cols = slice(p * w, (p + 1) * w)
        su_send[p, 0] = (bk[:, cols].astype(F32) * bv[:, cols].astype(F32)).astype(BF16)
        su_send[p, 1] = (bg[:, cols].astype(F32) * bq[:, cols].astype(F32)).astype(BF16)
    pl.semaphore_wait(barrier, n - 1 + nc - 1)

    for z in zpeers:
        part = fz.at[pl.ds(mz * per, per)]
        send(part, part, z_ss.at[z], z_rs.at[mz], {"chan": z})
    for p in peers:
        send(su_send.at[p], su.at[me], su_ss.at[p], su_rs.at[me], {"seq": p})
    for p in range(n):
        cols = slice(p * w, (p + 1) * w)
        s1_send[p] = (fk[:, cols].astype(F32) * fv[:, cols].astype(F32)).astype(BF16)
    for z in zpeers:
        arrived(fz.at[pl.ds(z * per, per)], z_ss.at[z], z_rs.at[z], {"chan": z})
    for p in peers:
        send(fz.at[p], rf.at[me], f_ss.at[p], f_rs.at[me], {"seq": p})
    for p in peers:
        send(s1_send.at[p], s1.at[me], s1_ss.at[p], s1_rs.at[me], {"seq": p})
    su[me] = su_send[me]
    s1[me] = s1_send[me]
    rf[me] = fz[me]

    def transform(dst, q, block):
        dst[q] = jnp.dot(fwd_t[...], block, preferred_element_type=F32)

    sign = 1.0 - 2.0 * lax.rem(lax.broadcasted_iota(jnp.int32, (rows, w), 0), 2).astype(F32)

    def windowed(src):
        spec_w[0] = src[0]
        for d in range(1, n):
            spec_w[d, :rows] = src[d, :rows] - sign * src[d - 1, rows:]
            spec_w[d, rows:] = src[d, rows:] + sign * src[d - 1, :rows]

    def products(src, corr):
        def tile(k, carry):
            re_at = pl.ds(pl.multiple_of(k * 8, 8), 8)
            im_at = pl.ds(pl.multiple_of(rows + k * 8, 8), 8)
            ar = [spec_w[d, re_at] for d in range(n)]
            ai = [spec_w[d, im_at] for d in range(n)]
            xr = [src[d, re_at] for d in range(n)]
            xi = [src[d, im_at] for d in range(n)]
            for b in range(n):
                terms = [(c - b, c) for c in range(b, n)] if corr else [(b - c, c) for c in range(b + 1)]
                re, im = None, None
                for d, c in terms:
                    if corr:
                        tr = ar[d] * xr[c] + ai[d] * xi[c]
                        ti = ar[d] * xi[c] - ai[d] * xr[c]
                    else:
                        tr = ar[d] * xr[c] - ai[d] * xi[c]
                        ti = ar[d] * xi[c] + ai[d] * xr[c]
                    re = tr if re is None else re + tr
                    im = ti if im is None else im + ti
                prod[b, re_at] = re
                prod[b, im_at] = im
            return carry

        lax.fori_loop(0, rows // 8, tile, 0)

    def inverse(b):
        return jnp.dot(inv_t[...], prod[b].astype(BF16), preferred_element_type=F32)

    def give_back(which):
        for b in range(n):
            c_send[which, b] = inverse(b).astype(BF16)
        for p in peers:
            send(c_send.at[which, p], c_recv.at[which, me], c_ss.at[which, p], c_rs.at[which, me], {"seq": p})
        c_recv[which, me] = c_send[which, me]

    total = jnp.zeros((1, w), F32)
    for q in [me] + peers:
        if q is not me:
            arrived(su.at[q], su_ss.at[q], su_rs.at[q], {"seq": q})
        transform(spec_s, q, su[q, 0])
        transform(spec_u, q, su[q, 1])
        total += jnp.sum(su[q, 0].astype(F32) * su[q, 1].astype(F32), axis=0, keepdims=True)
    k_send[...] = jnp.broadcast_to(total * scale, k_send.shape)
    for p in peers:
        send(k_send, k_recv.at[me], k_ss.at[p], k_rs.at[me], {"seq": p})
    k_recv[me] = k_send[...]

    windowed(spec_s)
    products(spec_u, True)
    for b in range(n):
        g_send[b] = (inverse(b) * scale).astype(BF16)
    for p in peers:
        send(g_send.at[p], rg.at[me], g_ss.at[p], g_rs.at[me], {"seq": p})
    rg[me] = g_send[me]

    for q in [me] + peers:
        if q is not me:
            arrived(rf.at[q], f_ss.at[q], f_rs.at[q], {"seq": q})
        transform(spec_f, q, rf[q])
    windowed(spec_f)
    products(spec_s, False)
    give_back(0)
    products(spec_u, True)
    give_back(1)

    for q in [me] + peers:
        if q is not me:
            arrived(s1.at[q], s1_ss.at[q], s1_rs.at[q], {"seq": q})
        transform(spec_s, q, s1[q])
    products(spec_s, False)
    give_back(2)

    for q in peers:
        arrived(rg.at[q], g_ss.at[q], g_rs.at[q], {"seq": q})
    for z in zpeers:
        send(rg.at[pl.ds(z * per, per)], zg.at[mz], y_ss.at[z], y_rs.at[mz], {"chan": z})

    for q in [me] + peers:
        at = lane(q)
        gain = skip[:, at]
        if q is not me:
            arrived(c_recv.at[0, q], c_ss.at[0, q], c_rs.at[0, q], {"seq": q})
        mixed = c_recv[0, q].astype(F32) + gain * su_send[q, 0].astype(F32)
        gq_o[:, at] = (bg[:, at].astype(F32) * mixed).astype(BF16)
    for q in [me] + peers:
        at = lane(q)
        gain = skip[:, at]
        if q is not me:
            arrived(c_recv.at[1, q], c_ss.at[1, q], c_rs.at[1, q], {"seq": q})
        through = c_recv[1, q].astype(F32) + gain * su_send[q, 1].astype(F32)
        gk_o[:, at] = (through * bv[:, at].astype(F32)).astype(BF16)
        gv_o[:, at] = (through * bk[:, at].astype(F32)).astype(BF16)
    for z in zpeers:
        arrived(zg.at[z], y_ss.at[z], y_rs.at[z], {"chan": z})
    for h in range(per):
        acc = rg[mz * per + h].astype(F32)
        for z in zpeers:
            acc += zg[z, h].astype(F32)
        gf_o[:, h * w:(h + 1) * w] = acc
    for q in peers:
        arrived(k_recv.at[q], k_ss.at[q], k_rs.at[q], {"seq": q})
    for q in range(n):
        gs_o[:, q * w:(q + 1) * w] = k_recv[q, 0:1]
    for q in [me] + peers:
        at = lane(q)
        gain = skip[:, at]
        if q is not me:
            arrived(c_recv.at[2, q], c_ss.at[2, q], c_rs.at[2, q], {"seq": q})
        mixed = c_recv[2, q].astype(F32) + gain * s1_send[q].astype(F32)
        out_o[:, at] = (fq[:, at].astype(F32) * mixed).astype(BF16)
    for c in started:
        c.wait_send()


def fused_device(n, nc, *args):
    fwd_q, filters, skip = args[0], args[7], args[8]
    rows, chan_width = fwd_q.shape
    w = chan_width // n
    per = filters.shape[1] // w
    scale = 1.0 / math.sqrt(rows * n)
    forward, inverse = (jnp.asarray(t, dtype=BF16) for t in block_tables(rows))
    wide = jax.ShapeDtypeStruct((rows, chan_width), BF16)
    vmem = pl.BlockSpec(memory_space=pltpu.VMEM)
    dma = pltpu.SemaphoreType.DMA
    block = (n, rows, w)
    spectrum = (n, 2 * rows, w)
    scratch = [
        pltpu.VMEM((n, 2, rows, w), BF16), pltpu.VMEM(block, BF16), pltpu.VMEM(block, BF16),
        pltpu.VMEM((n, 2, rows, w), BF16), pltpu.VMEM(block, BF16), pltpu.VMEM(block, BF16),
        *[pltpu.VMEM(spectrum, F32)] * 5,
        pltpu.VMEM((3,) + block, BF16), pltpu.VMEM((3,) + block, BF16),
        pltpu.VMEM(block, BF16), pltpu.VMEM(block, BF16), pltpu.VMEM((nc, per, rows, w), BF16),
        pltpu.VMEM((8, w), F32), pltpu.VMEM((n, 8, w), F32),
        dma((n,)), dma((n,)), dma((n,)), dma((n,)), dma((n,)), dma((n,)), dma((nc,)), dma((nc,)),
        dma((3, n)), dma((3, n)), dma((n,)), dma((n,)), dma((nc,)), dma((nc,)), dma((n,)), dma((n,)),
    ]
    outs = pl.pallas_call(
        functools.partial(kernel, n, nc, scale),
        out_shape=(
            wide, wide, wide, wide,
            jax.ShapeDtypeStruct(filters.shape, F32), jax.ShapeDtypeStruct((1, chan_width), F32),
        ),
        in_specs=[vmem] * 11,
        out_specs=(vmem,) * 6,
        scratch_shapes=scratch,
        compiler_params=pltpu.CompilerParams(
            collective_id=0, has_side_effects=True, vmem_limit_bytes=48 * 1024 * 1024
        ),
    )(*args[:8], skip.reshape(1, chan_width), forward, inverse)
    return outs[:5] + (outs[5].reshape(chan_width),)


def routed(*args):
    n, nc = lax.axis_size("seq"), lax.axis_size("chan")
    rows, chan_width = args[0].shape
    filter_width = args[7].shape[1]
    fits = chan_width % (n * LANES) == 0 and rows % 16 == 0
    if fits and filter_width * nc == chan_width and filter_width % (chan_width // n) == 0:
        return fused_device(n, nc, *args)
    return per_device(*args)


def solution(mesh):
    return jax.shard_map(
        routed,
        mesh=mesh,
        in_specs=(
            P("seq", "chan"),
            P("seq", "chan"),
            P("seq", "chan"),
            P("seq", "chan"),
            P("seq", "chan"),
            P("seq", "chan"),
            P("seq", "chan"),
            P("seq", "chan"),
            P("chan"),
        ),
        out_specs=(
            P("seq", "chan"),
            P("seq", "chan"),
            P("seq", "chan"),
            P("seq", "chan"),
            P("seq", "chan"),
            P("chan"),
        ),
        check_vma=False,
    )
```

```python
import functools
import math

import jax
import jax.numpy as jnp
import numpy as np
from jax import lax
from jax.experimental import pallas as pl
from jax.experimental.pallas import tpu as pltpu
from jax.sharding import PartitionSpec as P

HIGHEST = lax.Precision.HIGHEST
LANES = 128
MESH = pl.DeviceIdType.MESH
BF16 = jnp.bfloat16
F32 = jnp.float32


def index_ramp(total):
    return jnp.arange(total, dtype=jnp.int32)


def widened(values):
    return values.astype(jnp.float32)


def angles(out_index, in_index, period, sign):
    phase_steps = out_index[:, None] * in_index[None, :] % period
    phase = phase_steps.astype(jnp.float32) * (sign * 2.0 * math.pi / period)
    return (jnp.cos(phase), jnp.sin(phase))


def times_table(left, right):
    return (left[0] * right[0] - left[1] * right[1], left[0] * right[1] + left[1] * right[0])


def block_table(pair):
    cosine, sine_part = pair
    return jnp.stack([jnp.stack([cosine, -sine_part]), jnp.stack([sine_part, cosine])])


def product_of(left, right):
    return jnp.stack(
        [left[0] * right[0] - left[1] * right[1], left[0] * right[1] + left[1] * right[0]]
    )


def conj_product(left, right):
    return jnp.stack(
        [left[0] * right[0] + left[1] * right[1], left[0] * right[1] - left[1] * right[0]]
    )


def joined(left, right):
    return jnp.concatenate([left, right], axis=-1)


def factor(total):
    chosen = 1
    for candidate in range(1, total + 1):
        if candidate * candidate <= total and total % candidate == 0:
            chosen = candidate
    return chosen


def leading_section(values, seq_size):
    cosine, sine_part = angles(index_ramp(2 * seq_size), index_ramp(seq_size), 2 * seq_size, -1.0)
    table = jnp.stack([cosine, sine_part])
    return jnp.einsum("rkp,pmc->rkmc", table, values, precision=HIGHEST)


def trailing_section(values, seq_size, period):
    cosine, sine_part = angles(index_ramp(seq_size), index_ramp(2 * seq_size), 2 * seq_size, 1.0)
    table = jnp.stack([cosine, -sine_part]) * (1.0 / period)
    return jnp.einsum("rpk,rkmc->pmc", table, values, precision=HIGHEST)


def inner_forward(values, freq_keys, period):
    lead_size, row_count, chan_count = values.shape[1:]
    outer_size = factor(row_count)
    inner_size = row_count // outer_size
    values = values.reshape(2, lead_size, outer_size, inner_size, chan_count)
    first_twiddle = angles(freq_keys, index_ramp(row_count), period, -1.0)
    first_twiddle = tuple(
        (part.reshape(lead_size, outer_size, inner_size) for part in first_twiddle)
    )
    outer_dft = angles(index_ramp(outer_size), index_ramp(outer_size), outer_size, -1.0)
    outer_table = times_table(
        tuple((part[None, :, :, None] for part in outer_dft)),
        tuple((part[:, None, :, :] for part in first_twiddle)),
    )
    values = jnp.einsum("rsjxab,sjabc->rjxbc", block_table(outer_table), values, precision=HIGHEST)
    second_twiddle = angles(index_ramp(outer_size), index_ramp(inner_size), row_count, -1.0)
    inner_dft = angles(index_ramp(inner_size), index_ramp(inner_size), inner_size, -1.0)
    inner_table = times_table(
        tuple((part[None, :, :] for part in inner_dft)),
        tuple((part[:, None, :] for part in second_twiddle)),
    )
    return jnp.einsum("rsxyb,sjxbc->rjxyc", block_table(inner_table), values, precision=HIGHEST)


def inner_inverse(values, freq_keys, period):
    lead_size, outer_size, inner_size, chan_count = values.shape[1:]
    row_count = outer_size * inner_size
    second_twiddle = angles(index_ramp(outer_size), index_ramp(inner_size), row_count, 1.0)
    inner_dft = angles(index_ramp(inner_size), index_ramp(inner_size), inner_size, 1.0)
    inner_table = times_table(
        tuple((part[:, :, None] for part in second_twiddle)),
        tuple((part[None, :, :] for part in inner_dft)),
    )
    values = jnp.einsum("rsxby,sjxyc->rjxbc", block_table(inner_table), values, precision=HIGHEST)
    first_twiddle = angles(freq_keys, index_ramp(row_count), period, 1.0)
    first_twiddle = tuple(
        (part.reshape(lead_size, outer_size, inner_size) for part in first_twiddle)
    )
    outer_dft = angles(index_ramp(outer_size), index_ramp(outer_size), outer_size, 1.0)
    outer_table = times_table(
        tuple((part[:, :, :, None] for part in first_twiddle)),
        tuple((part[None, :, None, :] for part in outer_dft)),
    )
    values = jnp.einsum("rsjabx,sjxbc->rjabc", block_table(outer_table), values, precision=HIGHEST)
    return values.reshape(2, lead_size, row_count, chan_count)


def forward_local(signal_part, seq_size):
    seq_length, chan_count = signal_part.shape
    row_count = seq_length // seq_size
    values = leading_section(signal_part.reshape(seq_size, row_count, chan_count), seq_size)
    return inner_forward(values, index_ramp(2 * seq_size), 2 * seq_length)


def inverse_local(values, seq_size):
    lead_size, outer_size, inner_size, chan_count = values.shape[1:]
    row_count = outer_size * inner_size
    period = 2 * seq_size * row_count
    values = inner_inverse(values, index_ramp(2 * seq_size), period)
    return trailing_section(values, seq_size, period).reshape(seq_size * row_count, chan_count)


def filter_times_pair(spec_filter, spec_pair):
    shape_pair = spec_pair.shape
    width = spec_filter.shape[-1]
    pair_view = spec_pair.reshape(shape_pair[:-1] + (2, width))
    filter_view = spec_filter[..., None, :]
    return product_of(filter_view, pair_view).reshape(shape_pair)


def per_device(fwd_q, fwd_k, fwd_v, bwd_q, bwd_k, bwd_v, bwd_grad, filters, skip):
    row_count, chan_width = fwd_q.shape
    seq_size = lax.axis_size("seq")
    grad_scale = 1.0 / math.sqrt(row_count * seq_size)
    source = (widened(fwd_k) * widened(fwd_v)).astype(jnp.bfloat16)
    second_source = (widened(bwd_k) * widened(bwd_v)).astype(jnp.bfloat16)
    upstream = (widened(bwd_grad) * widened(bwd_q)).astype(jnp.bfloat16)
    skip_gain = widened(skip)
    filters_all = lax.all_gather(filters, "chan", axis=1, tiled=True)
    narrow = chan_width // seq_size
    local_first, local_second = (
        lax.all_to_all(source, "seq", split_axis=1, concat_axis=0, tiled=True),
        lax.all_to_all(second_source, "seq", split_axis=1, concat_axis=0, tiled=True),
    )
    local_filter = lax.all_to_all(filters_all, "seq", split_axis=1, concat_axis=0, tiled=True)
    local_up = lax.all_to_all(upstream, "seq", split_axis=1, concat_axis=0, tiled=True)
    spec_sources = forward_local(
        widened(jnp.concatenate([local_first, local_second], axis=1)), seq_size
    )
    spec_filter = forward_local(local_filter, seq_size)
    conv_local = inverse_local(filter_times_pair(spec_filter, spec_sources), seq_size)
    conv_first, conv_second = (
        lax.all_to_all(conv_local[:, :narrow], "seq", split_axis=0, concat_axis=1, tiled=True),
        lax.all_to_all(conv_local[:, narrow:], "seq", split_axis=0, concat_axis=1, tiled=True),
    )
    spec_up = forward_local(widened(local_up), seq_size)
    spec_second = spec_sources[..., narrow:]
    back_local = inverse_local(
        joined(conj_product(spec_filter, spec_up), conj_product(spec_second, spec_up)), seq_size
    )
    through_conv, filter_terms = (
        lax.all_to_all(back_local[:, :narrow], "seq", split_axis=0, concat_axis=1, tiled=True),
        lax.all_to_all(
            back_local[:, narrow:] * grad_scale, "seq", split_axis=0, concat_axis=1, tiled=True
        ),
    )
    grad_filter = lax.psum_scatter(filter_terms, "chan", scatter_dimension=1, tiled=True)
    source_wide = widened(source)
    second_wide = widened(second_source)
    upstream_wide = widened(upstream)
    mixed = conv_first + skip_gain * source_wide
    output = (widened(fwd_q) * mixed).astype(jnp.bfloat16)
    mixed_two = conv_second + skip_gain * second_wide
    grad_query = (widened(bwd_grad) * mixed_two).astype(jnp.bfloat16)
    through = through_conv + skip_gain * upstream_wide
    grad_key = (through * widened(bwd_v)).astype(jnp.bfloat16)
    grad_value = (through * widened(bwd_k)).astype(jnp.bfloat16)
    grad_skip = lax.psum(jnp.sum(upstream_wide * second_wide, axis=0) * grad_scale, "seq")
    return (output, grad_query, grad_key, grad_value, grad_filter, grad_skip)


def block_tables(rows):
    freq = 2 * np.arange(rows)[:, None] + 1
    phase = (freq * np.arange(rows)[None, :] % (4 * rows)) * (np.pi / (2 * rows))
    forward = np.concatenate([np.cos(phase), -np.sin(phase)], axis=0)
    inverse = np.concatenate([np.cos(phase), -np.sin(phase)], axis=0).T / rows
    return forward.astype(np.float32), inverse.astype(np.float32)


def kernel(
    n, nc, scale,
    fq_h, fk_h, fv_h, bq_h, bk_h, bv_h, bg_h, filt_h, skip_h, fwd_h, inv_h,
    out_h, gq_h, gk_h, gv_h, gf_h, gs_h,
    fq, fk, fv, bq, bk, bv, bg, filt, skip, fwd_t, inv_t, in_sem,
    out_o, gq_o, gk_o, gv_o, gf_o, gs_o, out_sem,
    su_send, s1_send, fz, su, s1, rf, spec_s, spec_u, spec_f, spec_w, prod,
    c_send, c_recv, g_send, rg, zg, k_send, k_recv,
    su_ss, su_rs, s1_ss, s1_rs, f_ss, f_rs, z_ss, z_rs, c_ss, c_rs, g_ss, g_rs, y_ss, y_rs, k_ss, k_rs,
):
    rows, chan_width = fq.shape
    w = chan_width // n
    per = filt.shape[1] // w
    me = lax.axis_index("seq")
    mz = lax.axis_index("chan")
    peers = [lax.rem(me + r, n) for r in range(1, n)]
    zpeers = [lax.rem(mz + r, nc) for r in range(1, nc)]
    started = []

    def lane(p):
        return pl.ds(pl.multiple_of(p * w, w), w)

    def copy(src, dst, ss, rs, to):
        return pltpu.make_async_remote_copy(
            src_ref=src, dst_ref=dst, send_sem=ss, recv_sem=rs, device_id=to, device_id_type=MESH
        )

    def send(src, dst, ss, rs, to):
        c = copy(src, dst, ss, rs, to)
        c.start()
        started.append(c)

    def arrived(buf, ss, rs, to):
        copy(buf, buf, ss, rs, to).wait_recv()

    loads = {}
    order = ((filt_h, filt), (bk_h, bk), (bv_h, bv), (bg_h, bg), (bq_h, bq), (fk_h, fk), (fv_h, fv))
    for at, (far, near) in enumerate(order + ((fwd_h, fwd_t), (inv_h, inv_t), (skip_h, skip), (fq_h, fq))):
        loads[id(near)] = pltpu.make_async_copy(far, near, in_sem.at[at])
        loads[id(near)].start()

    def loaded(*refs):
        for ref in refs:
            loads[id(ref)].wait()

    stores = []

    def store(near, far):
        c = pltpu.make_async_copy(near, far, out_sem.at[len(stores)])
        c.start()
        stores.append(c)

    barrier = pltpu.get_barrier_semaphore()
    for p in peers:
        pl.semaphore_signal(barrier, inc=1, device_id={"seq": p}, device_id_type=MESH)
    for z in zpeers:
        pl.semaphore_signal(barrier, inc=1, device_id={"chan": z}, device_id_type=MESH)

    def gate_block(p):
        at = lane(p)
        su_send[p, 0] = (bk[:, at].astype(F32) * bv[:, at].astype(F32)).astype(BF16)
        su_send[p, 1] = (bg[:, at].astype(F32) * bq[:, at].astype(F32)).astype(BF16)

    loaded(filt)
    for h in range(per):
        fz[mz * per + h] = filt[:, h * w:(h + 1) * w].astype(BF16)
    pl.semaphore_wait(barrier, n - 1 + nc - 1)
    for z in zpeers:
        part = fz.at[pl.ds(mz * per, per)]
        send(part, part, z_ss.at[z], z_rs.at[mz], {"chan": z})
    loaded(bk, bv, bg, bq)
    for p in peers:
        gate_block(p)
        send(su_send.at[p], su.at[me], su_ss.at[p], su_rs.at[me], {"seq": p})
    gate_block(me)
    su[me] = su_send[me]
    loaded(fk, fv)
    for p in range(n):
        cols = slice(p * w, (p + 1) * w)
        s1_send[p] = (fk[:, cols].astype(F32) * fv[:, cols].astype(F32)).astype(BF16)
    s1[me] = s1_send[me]
    loaded(fwd_t, inv_t)
    for z in zpeers:
        arrived(fz.at[pl.ds(z * per, per)], z_ss.at[z], z_rs.at[z], {"chan": z})
    for p in peers:
        send(fz.at[p], rf.at[me], f_ss.at[p], f_rs.at[me], {"seq": p})
    for p in peers:
        send(s1_send.at[p], s1.at[me], s1_ss.at[p], s1_rs.at[me], {"seq": p})
    rf[me] = fz[me]

    def transform(dst, q, block):
        dst[q] = jnp.dot(fwd_t[...], block, preferred_element_type=F32)

    sign = 1.0 - 2.0 * lax.rem(lax.broadcasted_iota(jnp.int32, (rows, w), 0), 2).astype(F32)

    def windowed(src):
        spec_w[0] = src[0]
        for d in range(1, n):
            spec_w[d, :rows] = src[d, :rows] - sign * src[d - 1, rows:]
            spec_w[d, rows:] = src[d, rows:] + sign * src[d - 1, :rows]

    def products(src, corr):
        def tile(k, carry):
            re_at = pl.ds(pl.multiple_of(k * 8, 8), 8)
            im_at = pl.ds(pl.multiple_of(rows + k * 8, 8), 8)
            ar = [spec_w[d, re_at] for d in range(n)]
            ai = [spec_w[d, im_at] for d in range(n)]
            xr = [src[d, re_at] for d in range(n)]
            xi = [src[d, im_at] for d in range(n)]
            for b in range(n):
                terms = [(c - b, c) for c in range(b, n)] if corr else [(b - c, c) for c in range(b + 1)]
                re, im = None, None
                for d, c in terms:
                    if corr:
                        tr = ar[d] * xr[c] + ai[d] * xi[c]
                        ti = ar[d] * xi[c] - ai[d] * xr[c]
                    else:
                        tr = ar[d] * xr[c] - ai[d] * xi[c]
                        ti = ar[d] * xi[c] + ai[d] * xr[c]
                    re = tr if re is None else re + tr
                    im = ti if im is None else im + ti
                prod[b, re_at] = re
                prod[b, im_at] = im
            return carry

        lax.fori_loop(0, rows // 8, tile, 0)

    def inverse(b):
        return jnp.dot(inv_t[...], prod[b].astype(BF16), preferred_element_type=F32)

    def give_back(which):
        for p in peers:
            c_send[which, p] = inverse(p).astype(BF16)
            send(c_send.at[which, p], c_recv.at[which, me], c_ss.at[which, p], c_rs.at[which, me], {"seq": p})
        c_recv[which, me] = inverse(me).astype(BF16)

    total = jnp.zeros((1, w), F32)
    for q in [me] + peers:
        if q is not me:
            arrived(su.at[q], su_ss.at[q], su_rs.at[q], {"seq": q})
        transform(spec_s, q, su[q, 0])
        transform(spec_u, q, su[q, 1])
        total += jnp.sum(su[q, 0].astype(F32) * su[q, 1].astype(F32), axis=0, keepdims=True)
    k_send[...] = jnp.broadcast_to(total * scale, k_send.shape)
    for p in peers:
        send(k_send, k_recv.at[me], k_ss.at[p], k_rs.at[me], {"seq": p})
    k_recv[me] = k_send[...]

    windowed(spec_s)
    products(spec_u, True)
    for p in peers:
        g_send[p] = (inverse(p) * scale).astype(BF16)
        send(g_send.at[p], rg.at[me], g_ss.at[p], g_rs.at[me], {"seq": p})
    rg[me] = (inverse(me) * scale).astype(BF16)

    for q in [me] + peers:
        if q is not me:
            arrived(rf.at[q], f_ss.at[q], f_rs.at[q], {"seq": q})
        transform(spec_f, q, rf[q])
    windowed(spec_f)
    products(spec_s, False)
    give_back(0)
    products(spec_u, True)
    give_back(1)

    for q in [me] + peers:
        if q is not me:
            arrived(s1.at[q], s1_ss.at[q], s1_rs.at[q], {"seq": q})
        transform(spec_s, q, s1[q])
    products(spec_s, False)
    give_back(2)

    for q in peers:
        arrived(rg.at[q], g_ss.at[q], g_rs.at[q], {"seq": q})
    for z in zpeers:
        send(rg.at[pl.ds(z * per, per)], zg.at[mz], y_ss.at[z], y_rs.at[mz], {"chan": z})

    loaded(skip, fq)
    for q in [me] + peers:
        at = lane(q)
        gain = skip[:, at]
        if q is not me:
            arrived(c_recv.at[0, q], c_ss.at[0, q], c_rs.at[0, q], {"seq": q})
        mixed = c_recv[0, q].astype(F32) + gain * su_send[q, 0].astype(F32)
        gq_o[:, at] = (bg[:, at].astype(F32) * mixed).astype(BF16)
    store(gq_o, gq_h)
    for q in [me] + peers:
        at = lane(q)
        gain = skip[:, at]
        if q is not me:
            arrived(c_recv.at[1, q], c_ss.at[1, q], c_rs.at[1, q], {"seq": q})
        through = c_recv[1, q].astype(F32) + gain * su_send[q, 1].astype(F32)
        gk_o[:, at] = (through * bv[:, at].astype(F32)).astype(BF16)
        gv_o[:, at] = (through * bk[:, at].astype(F32)).astype(BF16)
    store(gk_o, gk_h)
    store(gv_o, gv_h)
    for z in zpeers:
        arrived(zg.at[z], y_ss.at[z], y_rs.at[z], {"chan": z})
    for h in range(per):
        acc = rg[mz * per + h].astype(F32)
        for z in zpeers:
            acc += zg[z, h].astype(F32)
        gf_o[:, h * w:(h + 1) * w] = acc
    store(gf_o, gf_h)
    for q in peers:
        arrived(k_recv.at[q], k_ss.at[q], k_rs.at[q], {"seq": q})
    for q in range(n):
        gs_o[:, q * w:(q + 1) * w] = k_recv[q, 0:1]
    store(gs_o, gs_h)
    for q in [me] + peers:
        at = lane(q)
        gain = skip[:, at]
        if q is not me:
            arrived(c_recv.at[2, q], c_ss.at[2, q], c_rs.at[2, q], {"seq": q})
        mixed = c_recv[2, q].astype(F32) + gain * s1_send[q].astype(F32)
        out_o[:, at] = (fq[:, at].astype(F32) * mixed).astype(BF16)
    store(out_o, out_h)
    for c in started:
        c.wait_send()
    for c in stores:
        c.wait()


def store_all(*refs):
    count = len(refs) // 3
    far, out, near = refs[:count], refs[count:2 * count], refs[2 * count:-1]
    sems = refs[-1]
    loads = [pltpu.make_async_copy(far[i], near[i], sems.at[0, i]) for i in range(count)]
    stores = [pltpu.make_async_copy(near[i], out[i], sems.at[1, i]) for i in range(count)]
    for c in loads:
        c.start()
    for i in range(count):
        loads[i].wait()
        stores[i].start()
    for c in stores:
        c.wait()


def fused_device(n, nc, *args):
    fwd_q, filters, skip = args[0], args[7], args[8]
    rows, chan_width = fwd_q.shape
    w = chan_width // n
    per = filters.shape[1] // w
    scale = 1.0 / math.sqrt(rows * n)
    forward, inverse = (jnp.asarray(t, dtype=BF16) for t in block_tables(rows))
    wide = jax.ShapeDtypeStruct((rows, chan_width), BF16)
    results = [
        *[pltpu.VMEM((rows, chan_width), BF16)] * 4, pltpu.VMEM(filters.shape, F32), pltpu.VMEM((1, chan_width), F32),
    ]
    dma = pltpu.SemaphoreType.DMA
    block = (n, rows, w)
    spectrum = (n, 2 * rows, w)
    scratch = [
        *[pltpu.VMEM((rows, chan_width), BF16)] * 7, pltpu.VMEM(filters.shape, F32),
        pltpu.VMEM((1, chan_width), F32), pltpu.VMEM(forward.shape, BF16), pltpu.VMEM(inverse.shape, BF16),
        dma((11,)),
        *results, dma((6,)),
        pltpu.VMEM((n, 2, rows, w), BF16), pltpu.VMEM(block, BF16), pltpu.VMEM(block, BF16),
        pltpu.VMEM((n, 2, rows, w), BF16), pltpu.VMEM(block, BF16), pltpu.VMEM(block, BF16),
        *[pltpu.VMEM(spectrum, F32)] * 5,
        pltpu.VMEM((3,) + block, BF16), pltpu.VMEM((3,) + block, BF16),
        pltpu.VMEM(block, BF16), pltpu.VMEM(block, BF16), pltpu.VMEM((nc, per, rows, w), BF16),
        pltpu.VMEM((8, w), F32), pltpu.VMEM((n, 8, w), F32),
        dma((n,)), dma((n,)), dma((n,)), dma((n,)), dma((n,)), dma((n,)), dma((nc,)), dma((nc,)),
        dma((3, n)), dma((3, n)), dma((n,)), dma((n,)), dma((nc,)), dma((nc,)), dma((n,)), dma((n,)),
    ]
    full = 67_000_000
    hbm = pl.BlockSpec(memory_space=pltpu.HBM)
    outs = pl.pallas_call(
        functools.partial(kernel, n, nc, scale),
        out_shape=(
            wide, wide, wide, wide,
            jax.ShapeDtypeStruct(filters.shape, F32), jax.ShapeDtypeStruct((1, chan_width), F32),
        ),
        in_specs=[hbm] * 11,
        out_specs=(hbm,) * 6,
        scratch_shapes=scratch,
        compiler_params=pltpu.CompilerParams(
            collective_id=0, has_side_effects=True, vmem_limit_bytes=full
        ),
    )(*args[:8], skip.reshape(1, chan_width), forward, inverse)
    outs = pl.pallas_call(
        store_all,
        out_shape=tuple(jax.ShapeDtypeStruct(o.shape, o.dtype) for o in outs),
        in_specs=[hbm] * 6,
        out_specs=(hbm,) * 6,
        scratch_shapes=[*results, dma((2, 6))],
        compiler_params=pltpu.CompilerParams(vmem_limit_bytes=full),
    )(*outs)
    return tuple(outs[:5]) + (outs[5].reshape(chan_width),)


def routed(*args):
    n, nc = lax.axis_size("seq"), lax.axis_size("chan")
    rows, chan_width = args[0].shape
    filter_width = args[7].shape[1]
    fits = chan_width % (n * LANES) == 0 and rows % 16 == 0
    if fits and filter_width * nc == chan_width and filter_width % (chan_width // n) == 0:
        return fused_device(n, nc, *args)
    return per_device(*args)


def solution(mesh):
    return jax.shard_map(
        routed,
        mesh=mesh,
        in_specs=(
            P("seq", "chan"),
            P("seq", "chan"),
            P("seq", "chan"),
            P("seq", "chan"),
            P("seq", "chan"),
            P("seq", "chan"),
            P("seq", "chan"),
            P("seq", "chan"),
            P("chan"),
        ),
        out_specs=(
            P("seq", "chan"),
            P("seq", "chan"),
            P("seq", "chan"),
            P("seq", "chan"),
            P("seq", "chan"),
            P("chan"),
        ),
        check_vma=False,
    )
```

```python
import functools
import math

import jax
import jax.numpy as jnp
import numpy as np
from jax import lax
from jax.experimental import pallas as pl
from jax.experimental.pallas import tpu as pltpu
from jax.sharding import PartitionSpec as P

HIGHEST = lax.Precision.HIGHEST
LANES = 128
MESH = pl.DeviceIdType.MESH
BF16 = jnp.bfloat16
F32 = jnp.float32


def index_ramp(total):
    return jnp.arange(total, dtype=jnp.int32)


def widened(values):
    return values.astype(jnp.float32)


def angles(out_index, in_index, period, sign):
    phase_steps = out_index[:, None] * in_index[None, :] % period
    phase = phase_steps.astype(jnp.float32) * (sign * 2.0 * math.pi / period)
    return (jnp.cos(phase), jnp.sin(phase))


def times_table(left, right):
    return (left[0] * right[0] - left[1] * right[1], left[0] * right[1] + left[1] * right[0])


def block_table(pair):
    cosine, sine_part = pair
    return jnp.stack([jnp.stack([cosine, -sine_part]), jnp.stack([sine_part, cosine])])


def product_of(left, right):
    return jnp.stack(
        [left[0] * right[0] - left[1] * right[1], left[0] * right[1] + left[1] * right[0]]
    )


def conj_product(left, right):
    return jnp.stack(
        [left[0] * right[0] + left[1] * right[1], left[0] * right[1] - left[1] * right[0]]
    )


def joined(left, right):
    return jnp.concatenate([left, right], axis=-1)


def factor(total):
    chosen = 1
    for candidate in range(1, total + 1):
        if candidate * candidate <= total and total % candidate == 0:
            chosen = candidate
    return chosen


def leading_section(values, seq_size):
    cosine, sine_part = angles(index_ramp(2 * seq_size), index_ramp(seq_size), 2 * seq_size, -1.0)
    table = jnp.stack([cosine, sine_part])
    return jnp.einsum("rkp,pmc->rkmc", table, values, precision=HIGHEST)


def trailing_section(values, seq_size, period):
    cosine, sine_part = angles(index_ramp(seq_size), index_ramp(2 * seq_size), 2 * seq_size, 1.0)
    table = jnp.stack([cosine, -sine_part]) * (1.0 / period)
    return jnp.einsum("rpk,rkmc->pmc", table, values, precision=HIGHEST)


def inner_forward(values, freq_keys, period):
    lead_size, row_count, chan_count = values.shape[1:]
    outer_size = factor(row_count)
    inner_size = row_count // outer_size
    values = values.reshape(2, lead_size, outer_size, inner_size, chan_count)
    first_twiddle = angles(freq_keys, index_ramp(row_count), period, -1.0)
    first_twiddle = tuple(
        (part.reshape(lead_size, outer_size, inner_size) for part in first_twiddle)
    )
    outer_dft = angles(index_ramp(outer_size), index_ramp(outer_size), outer_size, -1.0)
    outer_table = times_table(
        tuple((part[None, :, :, None] for part in outer_dft)),
        tuple((part[:, None, :, :] for part in first_twiddle)),
    )
    values = jnp.einsum("rsjxab,sjabc->rjxbc", block_table(outer_table), values, precision=HIGHEST)
    second_twiddle = angles(index_ramp(outer_size), index_ramp(inner_size), row_count, -1.0)
    inner_dft = angles(index_ramp(inner_size), index_ramp(inner_size), inner_size, -1.0)
    inner_table = times_table(
        tuple((part[None, :, :] for part in inner_dft)),
        tuple((part[:, None, :] for part in second_twiddle)),
    )
    return jnp.einsum("rsxyb,sjxbc->rjxyc", block_table(inner_table), values, precision=HIGHEST)


def inner_inverse(values, freq_keys, period):
    lead_size, outer_size, inner_size, chan_count = values.shape[1:]
    row_count = outer_size * inner_size
    second_twiddle = angles(index_ramp(outer_size), index_ramp(inner_size), row_count, 1.0)
    inner_dft = angles(index_ramp(inner_size), index_ramp(inner_size), inner_size, 1.0)
    inner_table = times_table(
        tuple((part[:, :, None] for part in second_twiddle)),
        tuple((part[None, :, :] for part in inner_dft)),
    )
    values = jnp.einsum("rsxby,sjxyc->rjxbc", block_table(inner_table), values, precision=HIGHEST)
    first_twiddle = angles(freq_keys, index_ramp(row_count), period, 1.0)
    first_twiddle = tuple(
        (part.reshape(lead_size, outer_size, inner_size) for part in first_twiddle)
    )
    outer_dft = angles(index_ramp(outer_size), index_ramp(outer_size), outer_size, 1.0)
    outer_table = times_table(
        tuple((part[:, :, :, None] for part in first_twiddle)),
        tuple((part[None, :, None, :] for part in outer_dft)),
    )
    values = jnp.einsum("rsjabx,sjxbc->rjabc", block_table(outer_table), values, precision=HIGHEST)
    return values.reshape(2, lead_size, row_count, chan_count)


def forward_local(signal_part, seq_size):
    seq_length, chan_count = signal_part.shape
    row_count = seq_length // seq_size
    values = leading_section(signal_part.reshape(seq_size, row_count, chan_count), seq_size)
    return inner_forward(values, index_ramp(2 * seq_size), 2 * seq_length)


def inverse_local(values, seq_size):
    lead_size, outer_size, inner_size, chan_count = values.shape[1:]
    row_count = outer_size * inner_size
    period = 2 * seq_size * row_count
    values = inner_inverse(values, index_ramp(2 * seq_size), period)
    return trailing_section(values, seq_size, period).reshape(seq_size * row_count, chan_count)


def filter_times_pair(spec_filter, spec_pair):
    shape_pair = spec_pair.shape
    width = spec_filter.shape[-1]
    pair_view = spec_pair.reshape(shape_pair[:-1] + (2, width))
    filter_view = spec_filter[..., None, :]
    return product_of(filter_view, pair_view).reshape(shape_pair)


def per_device(fwd_q, fwd_k, fwd_v, bwd_q, bwd_k, bwd_v, bwd_grad, filters, skip):
    row_count, chan_width = fwd_q.shape
    seq_size = lax.axis_size("seq")
    grad_scale = 1.0 / math.sqrt(row_count * seq_size)
    source = (widened(fwd_k) * widened(fwd_v)).astype(jnp.bfloat16)
    second_source = (widened(bwd_k) * widened(bwd_v)).astype(jnp.bfloat16)
    upstream = (widened(bwd_grad) * widened(bwd_q)).astype(jnp.bfloat16)
    skip_gain = widened(skip)
    filters_all = lax.all_gather(filters, "chan", axis=1, tiled=True)
    narrow = chan_width // seq_size
    local_first, local_second = (
        lax.all_to_all(source, "seq", split_axis=1, concat_axis=0, tiled=True),
        lax.all_to_all(second_source, "seq", split_axis=1, concat_axis=0, tiled=True),
    )
    local_filter = lax.all_to_all(filters_all, "seq", split_axis=1, concat_axis=0, tiled=True)
    local_up = lax.all_to_all(upstream, "seq", split_axis=1, concat_axis=0, tiled=True)
    spec_sources = forward_local(
        widened(jnp.concatenate([local_first, local_second], axis=1)), seq_size
    )
    spec_filter = forward_local(local_filter, seq_size)
    conv_local = inverse_local(filter_times_pair(spec_filter, spec_sources), seq_size)
    conv_first, conv_second = (
        lax.all_to_all(conv_local[:, :narrow], "seq", split_axis=0, concat_axis=1, tiled=True),
        lax.all_to_all(conv_local[:, narrow:], "seq", split_axis=0, concat_axis=1, tiled=True),
    )
    spec_up = forward_local(widened(local_up), seq_size)
    spec_second = spec_sources[..., narrow:]
    back_local = inverse_local(
        joined(conj_product(spec_filter, spec_up), conj_product(spec_second, spec_up)), seq_size
    )
    through_conv, filter_terms = (
        lax.all_to_all(back_local[:, :narrow], "seq", split_axis=0, concat_axis=1, tiled=True),
        lax.all_to_all(
            back_local[:, narrow:] * grad_scale, "seq", split_axis=0, concat_axis=1, tiled=True
        ),
    )
    grad_filter = lax.psum_scatter(filter_terms, "chan", scatter_dimension=1, tiled=True)
    source_wide = widened(source)
    second_wide = widened(second_source)
    upstream_wide = widened(upstream)
    mixed = conv_first + skip_gain * source_wide
    output = (widened(fwd_q) * mixed).astype(jnp.bfloat16)
    mixed_two = conv_second + skip_gain * second_wide
    grad_query = (widened(bwd_grad) * mixed_two).astype(jnp.bfloat16)
    through = through_conv + skip_gain * upstream_wide
    grad_key = (through * widened(bwd_v)).astype(jnp.bfloat16)
    grad_value = (through * widened(bwd_k)).astype(jnp.bfloat16)
    grad_skip = lax.psum(jnp.sum(upstream_wide * second_wide, axis=0) * grad_scale, "seq")
    return (output, grad_query, grad_key, grad_value, grad_filter, grad_skip)


def block_tables(rows):
    freq = 2 * np.arange(rows)[:, None] + 1
    phase = (freq * np.arange(rows)[None, :] % (4 * rows)) * (np.pi / (2 * rows))
    forward = np.concatenate([np.cos(phase), -np.sin(phase)], axis=0)
    inverse = np.concatenate([np.cos(phase), -np.sin(phase)], axis=0).T / rows
    return forward.astype(np.float32), inverse.astype(np.float32)


def kernel(
    n, nc, scale,
    fq_h, fk_h, fv_h, bq_h, bk_h, bv_h, bg_h, filt_h, skip_h, fwd_h, inv_h,
    out_h, gq_h, gk_h, gv_h, gf_h, gs_h,
    fq, fk, fv, bq, bk, bv, bg, filt, skip, fwd_t, inv_t, in_sem,
    out_o, gq_o, gk_o, gv_o, gf_o, gs_o, out_sem,
    su_send, s1_send, fz, su, s1, rf, spec_s, spec_u, spec_f, spec_w, prod,
    c_send, c_recv, g_send, g_recv, g_sum, rg, zg, k_send, k_recv,
    su_ss, su_rs, s1_ss, s1_rs, f_ss, f_rs, z_ss, z_rs, c_ss, c_rs, g_ss, g_rs, y_ss, y_rs, k_ss, k_rs, x_ss, x_rs,
):
    rows, chan_width = fq.shape
    w = chan_width // n
    per = filt.shape[1] // w
    part_rows = rows // nc
    me = lax.axis_index("seq")
    mz = lax.axis_index("chan")
    peers = [lax.rem(me + r, n) for r in range(1, n)]
    zpeers = [lax.rem(mz + r, nc) for r in range(1, nc)]
    started = []

    def lane(p):
        return pl.ds(pl.multiple_of(p * w, w), w)

    def copy(src, dst, ss, rs, to):
        return pltpu.make_async_remote_copy(
            src_ref=src, dst_ref=dst, send_sem=ss, recv_sem=rs, device_id=to, device_id_type=MESH
        )

    def send(src, dst, ss, rs, to):
        c = copy(src, dst, ss, rs, to)
        c.start()
        started.append(c)

    def arrived(buf, ss, rs, to):
        copy(buf, buf, ss, rs, to).wait_recv()

    loads = {}
    order = ((filt_h, filt), (bk_h, bk), (bv_h, bv), (bg_h, bg), (bq_h, bq), (fk_h, fk), (fv_h, fv))
    for at, (far, near) in enumerate(order + ((fwd_h, fwd_t), (inv_h, inv_t), (skip_h, skip), (fq_h, fq))):
        loads[id(near)] = pltpu.make_async_copy(far, near, in_sem.at[at])
        loads[id(near)].start()

    def loaded(*refs):
        for ref in refs:
            loads[id(ref)].wait()

    stores = []

    def store(near, far):
        c = pltpu.make_async_copy(near, far, out_sem.at[len(stores)])
        c.start()
        stores.append(c)

    barrier = pltpu.get_barrier_semaphore()
    for p in peers:
        pl.semaphore_signal(barrier, inc=1, device_id={"seq": p}, device_id_type=MESH)
    for z in zpeers:
        pl.semaphore_signal(barrier, inc=1, device_id={"chan": z}, device_id_type=MESH)

    def transform(dst, q, block):
        dst[q] = jnp.dot(fwd_t[...], block, preferred_element_type=F32)

    def gate_block(p):
        at = lane(p)
        su_send[p, 0] = (bk[:, at].astype(F32) * bv[:, at].astype(F32)).astype(BF16)
        su_send[p, 1] = (bg[:, at].astype(F32) * bq[:, at].astype(F32)).astype(BF16)

    loaded(filt)
    for h in range(per):
        fz[mz * per + h] = filt[:, h * w:(h + 1) * w].astype(BF16)
    pl.semaphore_wait(barrier, n - 1 + nc - 1)
    for z in zpeers:
        part = fz.at[pl.ds(mz * per, per)]
        send(part, part, z_ss.at[z], z_rs.at[mz], {"chan": z})
    loaded(bk, bv, bg, bq)
    for p in peers:
        gate_block(p)
        send(su_send.at[p], su.at[me], su_ss.at[p], su_rs.at[me], {"seq": p})
    gate_block(me)
    su[me] = su_send[me]
    loaded(fk, fv)
    for p in range(n):
        cols = slice(p * w, (p + 1) * w)
        s1_send[p] = (fk[:, cols].astype(F32) * fv[:, cols].astype(F32)).astype(BF16)
    s1[me] = s1_send[me]
    loaded(fwd_t, inv_t)
    transform(spec_s, me, su[me, 0])
    transform(spec_u, me, su[me, 1])
    for z in zpeers:
        arrived(fz.at[pl.ds(z * per, per)], z_ss.at[z], z_rs.at[z], {"chan": z})
    for p in peers:
        send(fz.at[p], rf.at[me], f_ss.at[p], f_rs.at[me], {"seq": p})
    for p in peers:
        send(s1_send.at[p], s1.at[me], s1_ss.at[p], s1_rs.at[me], {"seq": p})
    rf[me] = fz[me]

    sign = 1.0 - 2.0 * lax.rem(lax.broadcasted_iota(jnp.int32, (rows, w), 0), 2).astype(F32)

    def windowed(src):
        spec_w[0] = src[0]
        for d in range(1, n):
            spec_w[d, :rows] = src[d, :rows] - sign * src[d - 1, rows:]
            spec_w[d, rows:] = src[d, rows:] + sign * src[d - 1, :rows]

    def products(src, corr):
        def tile(k, carry):
            re_at = pl.ds(pl.multiple_of(k * 8, 8), 8)
            im_at = pl.ds(pl.multiple_of(rows + k * 8, 8), 8)
            ar = [spec_w[d, re_at] for d in range(n)]
            ai = [spec_w[d, im_at] for d in range(n)]
            xr = [src[d, re_at] for d in range(n)]
            xi = [src[d, im_at] for d in range(n)]
            for b in range(n):
                terms = [(c - b, c) for c in range(b, n)] if corr else [(b - c, c) for c in range(b + 1)]
                re, im = None, None
                for d, c in terms:
                    if corr:
                        tr = ar[d] * xr[c] + ai[d] * xi[c]
                        ti = ar[d] * xi[c] - ai[d] * xr[c]
                    else:
                        tr = ar[d] * xr[c] - ai[d] * xi[c]
                        ti = ar[d] * xi[c] + ai[d] * xr[c]
                    re = tr if re is None else re + tr
                    im = ti if im is None else im + ti
                prod[b, re_at] = re
                prod[b, im_at] = im
            return carry

        lax.fori_loop(0, rows // 8, tile, 0)

    def inverse(b):
        return jnp.dot(inv_t[...], prod[b].astype(BF16), preferred_element_type=F32)

    def give_back(which):
        for p in peers:
            c_send[which, p] = inverse(p).astype(BF16)
            send(c_send.at[which, p], c_recv.at[which, me], c_ss.at[which, p], c_rs.at[which, me], {"seq": p})
        c_recv[which, me] = inverse(me).astype(BF16)

    total = jnp.zeros((1, w), F32)
    for q in [me] + peers:
        if q is not me:
            arrived(su.at[q], su_ss.at[q], su_rs.at[q], {"seq": q})
            transform(spec_s, q, su[q, 0])
            transform(spec_u, q, su[q, 1])
        total += jnp.sum(su[q, 0].astype(F32) * su[q, 1].astype(F32), axis=0, keepdims=True)
    k_send[...] = jnp.broadcast_to(total * scale, k_send.shape)
    for p in peers:
        send(k_send, k_recv.at[me], k_ss.at[p], k_rs.at[me], {"seq": p})
    k_recv[me] = k_send[...]

    windowed(spec_s)
    products(spec_u, True)
    for b in range(n):
        term = (inverse(b) * scale).astype(BF16)
        for z in range(nc):
            g_send[z, b] = term[z * part_rows:(z + 1) * part_rows]
    for z in zpeers:
        send(g_send.at[z], g_recv.at[mz], x_ss.at[z], x_rs.at[mz], {"chan": z})

    for q in [me] + peers:
        if q is not me:
            arrived(rf.at[q], f_ss.at[q], f_rs.at[q], {"seq": q})
        transform(spec_f, q, rf[q])
    windowed(spec_f)
    products(spec_s, False)
    give_back(0)
    products(spec_u, True)
    give_back(1)

    for q in [me] + peers:
        if q is not me:
            arrived(s1.at[q], s1_ss.at[q], s1_rs.at[q], {"seq": q})
        transform(spec_s, q, s1[q])
    products(spec_s, False)
    for z in zpeers:
        arrived(g_recv.at[z], x_ss.at[z], x_rs.at[z], {"chan": z})
    acc = g_send[mz].astype(F32)
    for z in zpeers:
        acc += g_recv[z].astype(F32)
    g_sum[...] = acc.astype(BF16)
    for p in peers:
        send(g_sum.at[p], rg.at[me], g_ss.at[p], g_rs.at[me], {"seq": p})
    rg[me] = g_sum[me]
    give_back(2)

    for q in peers:
        arrived(rg.at[q], g_ss.at[q], g_rs.at[q], {"seq": q})
    for z in zpeers:
        send(rg.at[pl.ds(z * per, per)], zg.at[mz], y_ss.at[z], y_rs.at[mz], {"chan": z})

    loaded(skip, fq)
    for q in [me] + peers:
        at = lane(q)
        gain = skip[:, at]
        if q is not me:
            arrived(c_recv.at[0, q], c_ss.at[0, q], c_rs.at[0, q], {"seq": q})
        mixed = c_recv[0, q].astype(F32) + gain * su_send[q, 0].astype(F32)
        gq_o[:, at] = (bg[:, at].astype(F32) * mixed).astype(BF16)
    store(gq_o, gq_h)
    for q in [me] + peers:
        at = lane(q)
        gain = skip[:, at]
        if q is not me:
            arrived(c_recv.at[1, q], c_ss.at[1, q], c_rs.at[1, q], {"seq": q})
        through = c_recv[1, q].astype(F32) + gain * su_send[q, 1].astype(F32)
        gk_o[:, at] = (through * bv[:, at].astype(F32)).astype(BF16)
        gv_o[:, at] = (through * bk[:, at].astype(F32)).astype(BF16)
    store(gk_o, gk_h)
    store(gv_o, gv_h)
    for z in zpeers:
        arrived(zg.at[z], y_ss.at[z], y_rs.at[z], {"chan": z})
    zg[mz] = rg[pl.ds(mz * per, per)]
    for z in range(nc):
        for h in range(per):
            gf_o[z * part_rows:(z + 1) * part_rows, h * w:(h + 1) * w] = zg[z, h].astype(F32)
    store(gf_o, gf_h)
    for q in peers:
        arrived(k_recv.at[q], k_ss.at[q], k_rs.at[q], {"seq": q})
    for q in range(n):
        gs_o[:, q * w:(q + 1) * w] = k_recv[q, 0:1]
    store(gs_o, gs_h)
    for q in [me] + peers:
        at = lane(q)
        gain = skip[:, at]
        if q is not me:
            arrived(c_recv.at[2, q], c_ss.at[2, q], c_rs.at[2, q], {"seq": q})
        mixed = c_recv[2, q].astype(F32) + gain * s1_send[q].astype(F32)
        out_o[:, at] = (fq[:, at].astype(F32) * mixed).astype(BF16)
    store(out_o, out_h)
    for c in started:
        c.wait_send()
    for c in stores:
        c.wait()


def store_all(*refs):
    count = len(refs) // 3
    far, out, near = refs[:count], refs[count:2 * count], refs[2 * count:-1]
    sems = refs[-1]
    loads = [pltpu.make_async_copy(far[i], near[i], sems.at[0, i]) for i in range(count)]
    stores = [pltpu.make_async_copy(near[i], out[i], sems.at[1, i]) for i in range(count)]
    for c in loads:
        c.start()
    for i in range(count):
        loads[i].wait()
        stores[i].start()
    for c in stores:
        c.wait()


def fused_device(n, nc, *args):
    fwd_q, filters, skip = args[0], args[7], args[8]
    rows, chan_width = fwd_q.shape
    w = chan_width // n
    per = filters.shape[1] // w
    scale = 1.0 / math.sqrt(rows * n)
    forward, inverse = (jnp.asarray(t, dtype=BF16) for t in block_tables(rows))
    wide = jax.ShapeDtypeStruct((rows, chan_width), BF16)
    results = [
        *[pltpu.VMEM((rows, chan_width), BF16)] * 4, pltpu.VMEM(filters.shape, F32), pltpu.VMEM((1, chan_width), F32),
    ]
    dma = pltpu.SemaphoreType.DMA
    block = (n, rows, w)
    part = (n, rows // nc, w)
    spectrum = (n, 2 * rows, w)
    scratch = [
        *[pltpu.VMEM((rows, chan_width), BF16)] * 7, pltpu.VMEM(filters.shape, F32),
        pltpu.VMEM((1, chan_width), F32), pltpu.VMEM(forward.shape, BF16), pltpu.VMEM(inverse.shape, BF16),
        dma((11,)),
        *results, dma((6,)),
        pltpu.VMEM((n, 2, rows, w), BF16), pltpu.VMEM(block, BF16), pltpu.VMEM(block, BF16),
        pltpu.VMEM((n, 2, rows, w), BF16), pltpu.VMEM(block, BF16), pltpu.VMEM(block, BF16),
        *[pltpu.VMEM(spectrum, F32)] * 5,
        pltpu.VMEM((3,) + block, BF16), pltpu.VMEM((3,) + block, BF16),
        pltpu.VMEM((nc,) + part, BF16), pltpu.VMEM((nc,) + part, BF16), pltpu.VMEM(part, BF16),
        pltpu.VMEM(part, BF16), pltpu.VMEM((nc, per, rows // nc, w), BF16),
        pltpu.VMEM((8, w), F32), pltpu.VMEM((n, 8, w), F32),
        dma((n,)), dma((n,)), dma((n,)), dma((n,)), dma((n,)), dma((n,)), dma((nc,)), dma((nc,)),
        dma((3, n)), dma((3, n)), dma((n,)), dma((n,)), dma((nc,)), dma((nc,)), dma((n,)), dma((n,)),
        dma((nc,)), dma((nc,)),
    ]
    full = 67_000_000
    hbm = pl.BlockSpec(memory_space=pltpu.HBM)
    outs = pl.pallas_call(
        functools.partial(kernel, n, nc, scale),
        out_shape=(
            wide, wide, wide, wide,
            jax.ShapeDtypeStruct(filters.shape, F32), jax.ShapeDtypeStruct((1, chan_width), F32),
        ),
        in_specs=[hbm] * 11,
        out_specs=(hbm,) * 6,
        scratch_shapes=scratch,
        compiler_params=pltpu.CompilerParams(
            collective_id=0, has_side_effects=True, vmem_limit_bytes=full
        ),
    )(*args[:8], skip.reshape(1, chan_width), forward, inverse)
    outs = pl.pallas_call(
        store_all,
        out_shape=tuple(jax.ShapeDtypeStruct(o.shape, o.dtype) for o in outs),
        in_specs=[hbm] * 6,
        out_specs=(hbm,) * 6,
        scratch_shapes=[*results, dma((2, 6))],
        compiler_params=pltpu.CompilerParams(vmem_limit_bytes=full),
    )(*outs)
    return tuple(outs[:5]) + (outs[5].reshape(chan_width),)


def routed(*args):
    n, nc = lax.axis_size("seq"), lax.axis_size("chan")
    rows, chan_width = args[0].shape
    filter_width = args[7].shape[1]
    fits = chan_width % (n * LANES) == 0 and rows % (16 * nc) == 0
    if fits and filter_width * nc == chan_width and filter_width % (chan_width // n) == 0:
        return fused_device(n, nc, *args)
    return per_device(*args)


def solution(mesh):
    return jax.shard_map(
        routed,
        mesh=mesh,
        in_specs=(
            P("seq", "chan"),
            P("seq", "chan"),
            P("seq", "chan"),
            P("seq", "chan"),
            P("seq", "chan"),
            P("seq", "chan"),
            P("seq", "chan"),
            P("seq", "chan"),
            P("chan"),
        ),
        out_specs=(
            P("seq", "chan"),
            P("seq", "chan"),
            P("seq", "chan"),
            P("seq", "chan"),
            P("seq", "chan"),
            P("chan"),
        ),
        check_vma=False,
    )
```

```python
import functools
import math

import jax
import jax.numpy as jnp
import numpy as np
from jax import lax
from jax.experimental import pallas as pl
from jax.experimental.pallas import tpu as pltpu
from jax.sharding import PartitionSpec as P

HIGHEST = lax.Precision.HIGHEST
LANES = 128
MESH = pl.DeviceIdType.MESH
BF16 = jnp.bfloat16
F32 = jnp.float32


def index_ramp(total):
    return jnp.arange(total, dtype=jnp.int32)


def widened(values):
    return values.astype(jnp.float32)


def angles(out_index, in_index, period, sign):
    phase_steps = out_index[:, None] * in_index[None, :] % period
    phase = phase_steps.astype(jnp.float32) * (sign * 2.0 * math.pi / period)
    return (jnp.cos(phase), jnp.sin(phase))


def times_table(left, right):
    return (left[0] * right[0] - left[1] * right[1], left[0] * right[1] + left[1] * right[0])


def block_table(pair):
    cosine, sine_part = pair
    return jnp.stack([jnp.stack([cosine, -sine_part]), jnp.stack([sine_part, cosine])])


def product_of(left, right):
    return jnp.stack(
        [left[0] * right[0] - left[1] * right[1], left[0] * right[1] + left[1] * right[0]]
    )


def conj_product(left, right):
    return jnp.stack(
        [left[0] * right[0] + left[1] * right[1], left[0] * right[1] - left[1] * right[0]]
    )


def joined(left, right):
    return jnp.concatenate([left, right], axis=-1)


def factor(total):
    chosen = 1
    for candidate in range(1, total + 1):
        if candidate * candidate <= total and total % candidate == 0:
            chosen = candidate
    return chosen


def leading_section(values, seq_size):
    cosine, sine_part = angles(index_ramp(2 * seq_size), index_ramp(seq_size), 2 * seq_size, -1.0)
    table = jnp.stack([cosine, sine_part])
    return jnp.einsum("rkp,pmc->rkmc", table, values, precision=HIGHEST)


def trailing_section(values, seq_size, period):
    cosine, sine_part = angles(index_ramp(seq_size), index_ramp(2 * seq_size), 2 * seq_size, 1.0)
    table = jnp.stack([cosine, -sine_part]) * (1.0 / period)
    return jnp.einsum("rpk,rkmc->pmc", table, values, precision=HIGHEST)


def inner_forward(values, freq_keys, period):
    lead_size, row_count, chan_count = values.shape[1:]
    outer_size = factor(row_count)
    inner_size = row_count // outer_size
    values = values.reshape(2, lead_size, outer_size, inner_size, chan_count)
    first_twiddle = angles(freq_keys, index_ramp(row_count), period, -1.0)
    first_twiddle = tuple(
        (part.reshape(lead_size, outer_size, inner_size) for part in first_twiddle)
    )
    outer_dft = angles(index_ramp(outer_size), index_ramp(outer_size), outer_size, -1.0)
    outer_table = times_table(
        tuple((part[None, :, :, None] for part in outer_dft)),
        tuple((part[:, None, :, :] for part in first_twiddle)),
    )
    values = jnp.einsum("rsjxab,sjabc->rjxbc", block_table(outer_table), values, precision=HIGHEST)
    second_twiddle = angles(index_ramp(outer_size), index_ramp(inner_size), row_count, -1.0)
    inner_dft = angles(index_ramp(inner_size), index_ramp(inner_size), inner_size, -1.0)
    inner_table = times_table(
        tuple((part[None, :, :] for part in inner_dft)),
        tuple((part[:, None, :] for part in second_twiddle)),
    )
    return jnp.einsum("rsxyb,sjxbc->rjxyc", block_table(inner_table), values, precision=HIGHEST)


def inner_inverse(values, freq_keys, period):
    lead_size, outer_size, inner_size, chan_count = values.shape[1:]
    row_count = outer_size * inner_size
    second_twiddle = angles(index_ramp(outer_size), index_ramp(inner_size), row_count, 1.0)
    inner_dft = angles(index_ramp(inner_size), index_ramp(inner_size), inner_size, 1.0)
    inner_table = times_table(
        tuple((part[:, :, None] for part in second_twiddle)),
        tuple((part[None, :, :] for part in inner_dft)),
    )
    values = jnp.einsum("rsxby,sjxyc->rjxbc", block_table(inner_table), values, precision=HIGHEST)
    first_twiddle = angles(freq_keys, index_ramp(row_count), period, 1.0)
    first_twiddle = tuple(
        (part.reshape(lead_size, outer_size, inner_size) for part in first_twiddle)
    )
    outer_dft = angles(index_ramp(outer_size), index_ramp(outer_size), outer_size, 1.0)
    outer_table = times_table(
        tuple((part[:, :, :, None] for part in first_twiddle)),
        tuple((part[None, :, None, :] for part in outer_dft)),
    )
    values = jnp.einsum("rsjabx,sjxbc->rjabc", block_table(outer_table), values, precision=HIGHEST)
    return values.reshape(2, lead_size, row_count, chan_count)


def forward_local(signal_part, seq_size):
    seq_length, chan_count = signal_part.shape
    row_count = seq_length // seq_size
    values = leading_section(signal_part.reshape(seq_size, row_count, chan_count), seq_size)
    return inner_forward(values, index_ramp(2 * seq_size), 2 * seq_length)


def inverse_local(values, seq_size):
    lead_size, outer_size, inner_size, chan_count = values.shape[1:]
    row_count = outer_size * inner_size
    period = 2 * seq_size * row_count
    values = inner_inverse(values, index_ramp(2 * seq_size), period)
    return trailing_section(values, seq_size, period).reshape(seq_size * row_count, chan_count)


def filter_times_pair(spec_filter, spec_pair):
    shape_pair = spec_pair.shape
    width = spec_filter.shape[-1]
    pair_view = spec_pair.reshape(shape_pair[:-1] + (2, width))
    filter_view = spec_filter[..., None, :]
    return product_of(filter_view, pair_view).reshape(shape_pair)


def per_device(fwd_q, fwd_k, fwd_v, bwd_q, bwd_k, bwd_v, bwd_grad, filters, skip):
    row_count, chan_width = fwd_q.shape
    seq_size = lax.axis_size("seq")
    grad_scale = 1.0 / math.sqrt(row_count * seq_size)
    source = (widened(fwd_k) * widened(fwd_v)).astype(jnp.bfloat16)
    second_source = (widened(bwd_k) * widened(bwd_v)).astype(jnp.bfloat16)
    upstream = (widened(bwd_grad) * widened(bwd_q)).astype(jnp.bfloat16)
    skip_gain = widened(skip)
    filters_all = lax.all_gather(filters, "chan", axis=1, tiled=True)
    narrow = chan_width // seq_size
    local_first, local_second = (
        lax.all_to_all(source, "seq", split_axis=1, concat_axis=0, tiled=True),
        lax.all_to_all(second_source, "seq", split_axis=1, concat_axis=0, tiled=True),
    )
    local_filter = lax.all_to_all(filters_all, "seq", split_axis=1, concat_axis=0, tiled=True)
    local_up = lax.all_to_all(upstream, "seq", split_axis=1, concat_axis=0, tiled=True)
    spec_sources = forward_local(
        widened(jnp.concatenate([local_first, local_second], axis=1)), seq_size
    )
    spec_filter = forward_local(local_filter, seq_size)
    conv_local = inverse_local(filter_times_pair(spec_filter, spec_sources), seq_size)
    conv_first, conv_second = (
        lax.all_to_all(conv_local[:, :narrow], "seq", split_axis=0, concat_axis=1, tiled=True),
        lax.all_to_all(conv_local[:, narrow:], "seq", split_axis=0, concat_axis=1, tiled=True),
    )
    spec_up = forward_local(widened(local_up), seq_size)
    spec_second = spec_sources[..., narrow:]
    back_local = inverse_local(
        joined(conj_product(spec_filter, spec_up), conj_product(spec_second, spec_up)), seq_size
    )
    through_conv, filter_terms = (
        lax.all_to_all(back_local[:, :narrow], "seq", split_axis=0, concat_axis=1, tiled=True),
        lax.all_to_all(
            back_local[:, narrow:] * grad_scale, "seq", split_axis=0, concat_axis=1, tiled=True
        ),
    )
    grad_filter = lax.psum_scatter(filter_terms, "chan", scatter_dimension=1, tiled=True)
    source_wide = widened(source)
    second_wide = widened(second_source)
    upstream_wide = widened(upstream)
    mixed = conv_first + skip_gain * source_wide
    output = (widened(fwd_q) * mixed).astype(jnp.bfloat16)
    mixed_two = conv_second + skip_gain * second_wide
    grad_query = (widened(bwd_grad) * mixed_two).astype(jnp.bfloat16)
    through = through_conv + skip_gain * upstream_wide
    grad_key = (through * widened(bwd_v)).astype(jnp.bfloat16)
    grad_value = (through * widened(bwd_k)).astype(jnp.bfloat16)
    grad_skip = lax.psum(jnp.sum(upstream_wide * second_wide, axis=0) * grad_scale, "seq")
    return (output, grad_query, grad_key, grad_value, grad_filter, grad_skip)


def block_tables(rows):
    freq = 2 * np.arange(rows)[:, None] + 1
    phase = (freq * np.arange(rows)[None, :] % (4 * rows)) * (np.pi / (2 * rows))
    forward = np.concatenate([np.cos(phase), -np.sin(phase)], axis=0)
    inverse = np.concatenate([np.cos(phase), -np.sin(phase)], axis=0).T / rows
    return forward.astype(np.float32), inverse.astype(np.float32)


def kernel(
    n, nc, scale,
    fq_h, fk_h, fv_h, bq_h, bk_h, bv_h, bg_h, filt_h, skip_h, fwd_h, inv_h,
    out_h, gq_h, gk_h, gv_h, gf_h, gs_h,
    fq, fk, fv, bq, bk, bv, bg, filt, skip, fwd_t, inv_t, in_sem,
    out_o, gq_o, gk_o, gv_o, gf_o, gs_o, out_sem,
    su_send, s1_send, fz, su, s1, rf, spec_s, spec_u, spec_f, spec_w, prod,
    c_send, c_recv, g_send, rg, zg, k_send, k_recv,
    su_ss, su_rs, s1_ss, s1_rs, f_ss, f_rs, z_ss, z_rs, c_ss, c_rs, g_ss, g_rs, y_ss, y_rs, k_ss, k_rs,
):
    rows, chan_width = fq.shape
    w = chan_width // n
    per = filt.shape[1] // w
    me = lax.axis_index("seq")
    mz = lax.axis_index("chan")
    peers = [lax.rem(me + r, n) for r in range(1, n)]
    senders = peers[::-1]
    zpeers = [lax.rem(mz + r, nc) for r in range(1, nc)]
    started = []

    def lane(p):
        return pl.ds(pl.multiple_of(p * w, w), w)

    def copy(src, dst, ss, rs, to):
        return pltpu.make_async_remote_copy(
            src_ref=src, dst_ref=dst, send_sem=ss, recv_sem=rs, device_id=to, device_id_type=MESH
        )

    def send(src, dst, ss, rs, to):
        c = copy(src, dst, ss, rs, to)
        c.start()
        started.append(c)

    def arrived(buf, ss, rs, to):
        copy(buf, buf, ss, rs, to).wait_recv()

    loads = {}
    order = ((filt_h, filt), (bk_h, bk), (bv_h, bv), (bg_h, bg), (bq_h, bq), (fk_h, fk), (fv_h, fv))
    for at, (far, near) in enumerate(order + ((fwd_h, fwd_t), (inv_h, inv_t), (skip_h, skip), (fq_h, fq))):
        loads[id(near)] = pltpu.make_async_copy(far, near, in_sem.at[at])
        loads[id(near)].start()

    def loaded(*refs):
        for ref in refs:
            loads[id(ref)].wait()

    stores = []

    def store(near, far):
        c = pltpu.make_async_copy(near, far, out_sem.at[len(stores)])
        c.start()
        stores.append(c)

    barrier = pltpu.get_barrier_semaphore()
    for p in peers:
        pl.semaphore_signal(barrier, inc=1, device_id={"seq": p}, device_id_type=MESH)
    for z in zpeers:
        pl.semaphore_signal(barrier, inc=1, device_id={"chan": z}, device_id_type=MESH)

    def transform(dst, q, block):
        dst[q] = jnp.dot(fwd_t[...], block, preferred_element_type=F32)

    def gate_block(p):
        at = lane(p)
        su_send[p, 0] = (bk[:, at].astype(F32) * bv[:, at].astype(F32)).astype(BF16)
        su_send[p, 1] = (bg[:, at].astype(F32) * bq[:, at].astype(F32)).astype(BF16)

    loaded(filt)
    for h in range(per):
        fz[mz * per + h] = filt[:, h * w:(h + 1) * w].astype(BF16)
    pl.semaphore_wait(barrier, n - 1 + nc - 1)
    for z in zpeers:
        part = fz.at[pl.ds(mz * per, per)]
        send(part, part, z_ss.at[z], z_rs.at[mz], {"chan": z})
    loaded(bk, bv, bg, bq)
    for p in peers:
        gate_block(p)
        send(su_send.at[p], su.at[me], su_ss.at[p], su_rs.at[me], {"seq": p})
    gate_block(me)
    su[me] = su_send[me]
    loaded(fk, fv)
    for p in range(n):
        cols = slice(p * w, (p + 1) * w)
        s1_send[p] = (fk[:, cols].astype(F32) * fv[:, cols].astype(F32)).astype(BF16)
    s1[me] = s1_send[me]
    loaded(fwd_t, inv_t)
    transform(spec_s, me, su[me, 0])
    transform(spec_u, me, su[me, 1])
    for z in zpeers:
        arrived(fz.at[pl.ds(z * per, per)], z_ss.at[z], z_rs.at[z], {"chan": z})
    for p in peers:
        send(fz.at[p], rf.at[me], f_ss.at[p], f_rs.at[me], {"seq": p})
    for p in peers:
        send(s1_send.at[p], s1.at[me], s1_ss.at[p], s1_rs.at[me], {"seq": p})
    rf[me] = fz[me]

    sign = 1.0 - 2.0 * lax.rem(lax.broadcasted_iota(jnp.int32, (rows, w), 0), 2).astype(F32)

    def windowed(src):
        spec_w[0] = src[0]
        for d in range(1, n):
            spec_w[d, :rows] = src[d, :rows] - sign * src[d - 1, rows:]
            spec_w[d, rows:] = src[d, rows:] + sign * src[d - 1, :rows]

    def products(src, corr):
        def tile(k, carry):
            re_at = pl.ds(pl.multiple_of(k * 8, 8), 8)
            im_at = pl.ds(pl.multiple_of(rows + k * 8, 8), 8)
            ar = [spec_w[d, re_at] for d in range(n)]
            ai = [spec_w[d, im_at] for d in range(n)]
            xr = [src[d, re_at] for d in range(n)]
            xi = [src[d, im_at] for d in range(n)]
            for b in range(n):
                terms = [(c - b, c) for c in range(b, n)] if corr else [(b - c, c) for c in range(b + 1)]
                re, im = None, None
                for d, c in terms:
                    if corr:
                        tr = ar[d] * xr[c] + ai[d] * xi[c]
                        ti = ar[d] * xi[c] - ai[d] * xr[c]
                    else:
                        tr = ar[d] * xr[c] - ai[d] * xi[c]
                        ti = ar[d] * xi[c] + ai[d] * xr[c]
                    re = tr if re is None else re + tr
                    im = ti if im is None else im + ti
                prod[b, re_at] = re
                prod[b, im_at] = im
            return carry

        lax.fori_loop(0, rows // 8, tile, 0)

    def inverse(b):
        return jnp.dot(inv_t[...], prod[b].astype(BF16), preferred_element_type=F32)

    def give_back(which):
        for p in peers:
            c_send[which, p] = inverse(p).astype(BF16)
            send(c_send.at[which, p], c_recv.at[which, me], c_ss.at[which, p], c_rs.at[which, me], {"seq": p})
        c_recv[which, me] = inverse(me).astype(BF16)

    total = jnp.zeros((1, w), F32)
    for q in [me] + senders:
        if q is not me:
            arrived(su.at[q], su_ss.at[q], su_rs.at[q], {"seq": q})
            transform(spec_s, q, su[q, 0])
            transform(spec_u, q, su[q, 1])
        total += jnp.sum(su[q, 0].astype(F32) * su[q, 1].astype(F32), axis=0, keepdims=True)
    k_send[...] = jnp.broadcast_to(total * scale, k_send.shape)
    for p in peers:
        send(k_send, k_recv.at[me], k_ss.at[p], k_rs.at[me], {"seq": p})
    k_recv[me] = k_send[...]

    windowed(spec_s)
    products(spec_u, True)
    for p in peers:
        g_send[p] = (inverse(p) * scale).astype(BF16)
        send(g_send.at[p], rg.at[me], g_ss.at[p], g_rs.at[me], {"seq": p})
    rg[me] = (inverse(me) * scale).astype(BF16)

    for q in [me] + senders:
        if q is not me:
            arrived(rf.at[q], f_ss.at[q], f_rs.at[q], {"seq": q})
        transform(spec_f, q, rf[q])
    windowed(spec_f)
    products(spec_s, False)
    give_back(0)
    products(spec_u, True)
    give_back(1)

    for q in [me] + senders:
        if q is not me:
            arrived(s1.at[q], s1_ss.at[q], s1_rs.at[q], {"seq": q})
        transform(spec_s, q, s1[q])
    products(spec_s, False)
    give_back(2)

    for q in senders:
        arrived(rg.at[q], g_ss.at[q], g_rs.at[q], {"seq": q})
    for z in zpeers:
        send(rg.at[pl.ds(z * per, per)], zg.at[mz], y_ss.at[z], y_rs.at[mz], {"chan": z})

    loaded(skip, fq)
    for q in [me] + senders:
        at = lane(q)
        gain = skip[:, at]
        if q is not me:
            arrived(c_recv.at[0, q], c_ss.at[0, q], c_rs.at[0, q], {"seq": q})
        mixed = c_recv[0, q].astype(F32) + gain * su_send[q, 0].astype(F32)
        gq_o[:, at] = (bg[:, at].astype(F32) * mixed).astype(BF16)
    store(gq_o, gq_h)
    for q in [me] + senders:
        at = lane(q)
        gain = skip[:, at]
        if q is not me:
            arrived(c_recv.at[1, q], c_ss.at[1, q], c_rs.at[1, q], {"seq": q})
        through = c_recv[1, q].astype(F32) + gain * su_send[q, 1].astype(F32)
        gk_o[:, at] = (through * bv[:, at].astype(F32)).astype(BF16)
        gv_o[:, at] = (through * bk[:, at].astype(F32)).astype(BF16)
    store(gk_o, gk_h)
    store(gv_o, gv_h)
    for z in zpeers:
        arrived(zg.at[z], y_ss.at[z], y_rs.at[z], {"chan": z})
    for h in range(per):
        acc = rg[mz * per + h].astype(F32)
        for z in zpeers:
            acc += zg[z, h].astype(F32)
        gf_o[:, h * w:(h + 1) * w] = acc
    store(gf_o, gf_h)
    for q in senders:
        arrived(k_recv.at[q], k_ss.at[q], k_rs.at[q], {"seq": q})
    for q in range(n):
        gs_o[:, q * w:(q + 1) * w] = k_recv[q, 0:1]
    store(gs_o, gs_h)
    for q in [me] + senders:
        at = lane(q)
        gain = skip[:, at]
        if q is not me:
            arrived(c_recv.at[2, q], c_ss.at[2, q], c_rs.at[2, q], {"seq": q})
        mixed = c_recv[2, q].astype(F32) + gain * s1_send[q].astype(F32)
        out_o[:, at] = (fq[:, at].astype(F32) * mixed).astype(BF16)
    store(out_o, out_h)
    for c in started:
        c.wait_send()
    for c in stores:
        c.wait()


def store_all(*refs):
    count = len(refs) // 3
    far, out, near = refs[:count], refs[count:2 * count], refs[2 * count:-1]
    sems = refs[-1]
    loads = [pltpu.make_async_copy(far[i], near[i], sems.at[0, i]) for i in range(count)]
    stores = [pltpu.make_async_copy(near[i], out[i], sems.at[1, i]) for i in range(count)]
    for c in loads:
        c.start()
    for i in range(count):
        loads[i].wait()
        stores[i].start()
    for c in stores:
        c.wait()


def fused_device(n, nc, *args):
    fwd_q, filters, skip = args[0], args[7], args[8]
    rows, chan_width = fwd_q.shape
    w = chan_width // n
    per = filters.shape[1] // w
    scale = 1.0 / math.sqrt(rows * n)
    forward, inverse = (jnp.asarray(t, dtype=BF16) for t in block_tables(rows))
    wide = jax.ShapeDtypeStruct((rows, chan_width), BF16)
    results = [
        *[pltpu.VMEM((rows, chan_width), BF16)] * 4, pltpu.VMEM(filters.shape, F32), pltpu.VMEM((1, chan_width), F32),
    ]
    dma = pltpu.SemaphoreType.DMA
    block = (n, rows, w)
    spectrum = (n, 2 * rows, w)
    scratch = [
        *[pltpu.VMEM((rows, chan_width), BF16)] * 7, pltpu.VMEM(filters.shape, F32),
        pltpu.VMEM((1, chan_width), F32), pltpu.VMEM(forward.shape, BF16), pltpu.VMEM(inverse.shape, BF16),
        dma((11,)),
        *results, dma((6,)),
        pltpu.VMEM((n, 2, rows, w), BF16), pltpu.VMEM(block, BF16), pltpu.VMEM(block, BF16),
        pltpu.VMEM((n, 2, rows, w), BF16), pltpu.VMEM(block, BF16), pltpu.VMEM(block, BF16),
        *[pltpu.VMEM(spectrum, F32)] * 5,
        pltpu.VMEM((3,) + block, BF16), pltpu.VMEM((3,) + block, BF16),
        pltpu.VMEM(block, BF16), pltpu.VMEM(block, BF16), pltpu.VMEM((nc, per, rows, w), BF16),
        pltpu.VMEM((8, w), F32), pltpu.VMEM((n, 8, w), F32),
        dma((n,)), dma((n,)), dma((n,)), dma((n,)), dma((n,)), dma((n,)), dma((nc,)), dma((nc,)),
        dma((3, n)), dma((3, n)), dma((n,)), dma((n,)), dma((nc,)), dma((nc,)), dma((n,)), dma((n,)),
    ]
    full = 67_000_000
    hbm = pl.BlockSpec(memory_space=pltpu.HBM)
    outs = pl.pallas_call(
        functools.partial(kernel, n, nc, scale),
        out_shape=(
            wide, wide, wide, wide,
            jax.ShapeDtypeStruct(filters.shape, F32), jax.ShapeDtypeStruct((1, chan_width), F32),
        ),
        in_specs=[hbm] * 11,
        out_specs=(hbm,) * 6,
        scratch_shapes=scratch,
        compiler_params=pltpu.CompilerParams(
            collective_id=0, has_side_effects=True, vmem_limit_bytes=full
        ),
    )(*args[:8], skip.reshape(1, chan_width), forward, inverse)
    outs = pl.pallas_call(
        store_all,
        out_shape=tuple(jax.ShapeDtypeStruct(o.shape, o.dtype) for o in outs),
        in_specs=[hbm] * 6,
        out_specs=(hbm,) * 6,
        scratch_shapes=[*results, dma((2, 6))],
        compiler_params=pltpu.CompilerParams(vmem_limit_bytes=full),
    )(*outs)
    return tuple(outs[:5]) + (outs[5].reshape(chan_width),)


def routed(*args):
    n, nc = lax.axis_size("seq"), lax.axis_size("chan")
    rows, chan_width = args[0].shape
    filter_width = args[7].shape[1]
    fits = chan_width % (n * LANES) == 0 and rows % 16 == 0
    if fits and filter_width * nc == chan_width and filter_width % (chan_width // n) == 0:
        return fused_device(n, nc, *args)
    return per_device(*args)


def solution(mesh):
    return jax.shard_map(
        routed,
        mesh=mesh,
        in_specs=(
            P("seq", "chan"),
            P("seq", "chan"),
            P("seq", "chan"),
            P("seq", "chan"),
            P("seq", "chan"),
            P("seq", "chan"),
            P("seq", "chan"),
            P("seq", "chan"),
            P("chan"),
        ),
        out_specs=(
            P("seq", "chan"),
            P("seq", "chan"),
            P("seq", "chan"),
            P("seq", "chan"),
            P("seq", "chan"),
            P("chan"),
        ),
        check_vma=False,
    )
```
